32 devices in a mesh: pair: 8 (over z, core), orb: 4 (over y, x).
Axes of the slice: x: 2, y: 2, z: 4, core: 2. Of those that a mesh axis runs over, the one named last changes fastest.
Arguments:
- amplitudes: float32 [128, 128, 128], P(('pair', 'orb')), may hold values from -3 to 3
- couple: int32 [128, 16], P(('pair', 'orb')), may hold values from 0 to 127, as said below
- occ_first: int32 [128], P('pair'), may hold values from 0 to 31, as said below
- occ_second: int32 [128], P('pair'), may hold values from 0 to 31, as said below
- couple_intersection: bfloat16 [128, 16, 128, 128], P(('pair', 'orb')), may hold values from -0.375 to 0.375
- pno_maps: bfloat16 [128, 2, 128, 128], P('pair'), may hold values from -0.5 to 0.5
- orbital_blocks: bfloat16 [32, 512, 128], P('pair', 'orb'), may hold values from -2 to 2
- pno_energy: float32 [128, 128], P(('pair', 'orb')), may hold values from 0.5 to 2.5
- occ_energy: float32 [32], replicated, may hold values from -1.5 to -0.3
Outputs:
- new_amplitudes: float32 [128, 128, 128], P(('pair', 'orb'))
- dressed: float32 [32, 512, 128], P('pair', 'orb')
The draws below stay inside these ranges and needn't reach their ends.
Inputs may be any that keep to these rules, and one draw needn't show every extreme that they name: `couple`: every listed partner of a pair lies in the same pair group as the pair (pairs g * 16 to (g + 1) * 16 - 1 form group g). `occ_first`: the pairs of group g have first orbitals in g * 4 to (g + 1) * 4 - 1. `occ_second`: the pairs of group g have second orbitals among the orbitals of groups g - 1 to g + 1, counted modulo 8 (group h holds orbitals h * 4 to (h + 1) * 4 - 1).
All inputs are finite; a program needn't handle non-finite values.
Results may differ from the reference program's by a relative error of at most 0.014.
Values may be sent and summed in bfloat16 or wider, within the bound.
A program may use at most 64 MiB of HBM per device.

```python
import math
import jax
import jax.numpy as jnp
from jax import lax

P_SIZE = 128
Q = 512
ORB_DEV = 4
KC = 16
REACH = 1
ITERS = 2
PAIR_GRP = 16
NPAIR = 128
NORB = 32
N_ORB = 4


def draw_couple(key, part):
    group_ids = jnp.arange(NPAIR, dtype=jnp.int32) // PAIR_GRP
    picked = jax.random.randint(jax.random.fold_in(key, 1), (NPAIR, KC), 0, PAIR_GRP, dtype=jnp.int32)
    return group_ids[:, None] * PAIR_GRP + picked


def draw_occ_first(key, part):
    group_ids = jnp.arange(NPAIR, dtype=jnp.int32) // PAIR_GRP
    picked = jax.random.randint(jax.random.fold_in(key, 3), (NPAIR,), 0, ORB_DEV, dtype=jnp.int32)
    return group_ids * ORB_DEV + picked


def draw_occ_second(key, part):
    groups = NPAIR // PAIR_GRP
    key_step, key_local = jax.random.split(jax.random.fold_in(key, 7), 2)
    steps_drawn = jax.random.randint(key_step, (groups, PAIR_GRP), 0, 2 * REACH + 1, dtype=jnp.int32)
    column = jnp.arange(PAIR_GRP, dtype=jnp.int32)[None, :]
    steps_drawn = jnp.where(column < 2 * REACH + 1, column, steps_drawn)
    group_ids = jnp.arange(groups, dtype=jnp.int32)[:, None]
    owner_ids = (group_ids + steps_drawn - REACH + groups) % groups
    local_ids = jax.random.randint(key_local, (groups, PAIR_GRP), 0, ORB_DEV, dtype=jnp.int32)
    return (owner_ids * ORB_DEV + local_ids).reshape(NPAIR)


def block_levels(own_key, extent, cuts, least, top_value):
    def one(axis_at, parts):
        heights = jax.random.uniform(jax.random.fold_in(jax.random.fold_in(own_key, 6), axis_at), (parts,), jnp.float32, least / len(cuts), top_value / len(cuts))
        return jnp.repeat(jnp.exp(heights), extent[axis_at] // parts).reshape((-1,) + (1,) * (len(extent) - axis_at - 1))

    factor_of = one(*cuts[0])
    for cut in cuts[1:]:
        factor_of = factor_of * one(*cut)
    return factor_of


def noise(rng, shape, width, most, cuts=(), kind=jnp.bfloat16):
    array = jax.random.normal(rng, shape, jnp.float32) * width
    if len(cuts) > 0:
        array = block_levels(rng, shape, cuts, -0.22, 0.18) * array
    return jnp.clip(array, min=-most, max=most).astype(kind)


def setup_inputs(seed: int = 0) -> dict:
    seeds = jax.random.split(jax.random.key(seed), 10)
    amplitudes = noise(seeds[0], (NPAIR, P_SIZE, P_SIZE), 0.5, 3.0, ((0, 32),), jnp.float32)
    couple = draw_couple(jax.random.fold_in(seeds[9], 71), 0)
    occ_first = draw_occ_first(jax.random.fold_in(seeds[9], 71), 0)
    occ_second = draw_occ_second(jax.random.fold_in(seeds[9], 71), 0)
    couple_intersection = noise(seeds[4], (NPAIR, KC, P_SIZE, P_SIZE), (2 * P_SIZE) ** -0.5, 0.375, ((0, 32),))
    pno_maps = noise(seeds[5], (NPAIR, 2, P_SIZE, P_SIZE), P_SIZE ** -0.5, 0.5, ((0, 8),))
    orbital_blocks = noise(seeds[6], (NORB, Q, P_SIZE), 0.3, 2.0, ((0, 8), (1, 4)))
    pno_energy = jnp.clip(jnp.exp(math.log(2.5) - 1.609438 * jax.random.uniform(seeds[7], (NPAIR, P_SIZE), jnp.float32) ** block_levels(seeds[7], (NPAIR, P_SIZE), ((0, 32),), -0.2, 0.2)), 0.5, 2.5)
    occ_energy = jnp.clip(jax.random.uniform(seeds[8], (NORB,), jnp.float32, -1.5, -0.3), -1.5, -0.3)
    return dict(amplitudes=amplitudes, couple=couple, occ_first=occ_first, occ_second=occ_second, couple_intersection=couple_intersection, pno_maps=pno_maps, orbital_blocks=orbital_blocks, pno_energy=pno_energy, occ_energy=occ_energy)


dress_scale = 0.015


def as_float(values):
    return values.astype(jnp.float32)


def reference(amplitudes, couple, occ_first, occ_second, couple_intersection, pno_maps, orbital_blocks, pno_energy, occ_energy):
    slice_rows = Q // N_ORB
    block_total = NPAIR // PAIR_GRP
    denominator = pno_energy[:, :, None] + pno_energy[:, None, :]
    denominator = denominator - occ_energy[occ_first][:, None, None] - occ_energy[occ_second][:, None, None]
    bare_blocks = as_float(orbital_blocks)
    dressed = bare_blocks
    amps_now = amplitudes
    highest = lax.Precision.HIGHEST
    for iteration in range(ITERS):
        amp_half = amps_now.astype(jnp.bfloat16)
        block_half = dressed.astype(jnp.bfloat16)

        def one_block(fitted, block_index):
            first_row = (block_index * PAIR_GRP).astype(jnp.int32)
            first_ids = lax.dynamic_slice_in_dim(occ_first, first_row, PAIR_GRP)
            second_ids = lax.dynamic_slice_in_dim(occ_second, first_row, PAIR_GRP)
            pair_maps = as_float(lax.dynamic_slice_in_dim(pno_maps, first_row, PAIR_GRP))
            first_proj = jnp.einsum("pqa,pab->pqb", as_float(block_half[first_ids]), pair_maps[:, 0], precision=highest).astype(jnp.bfloat16)
            second_proj = jnp.einsum("pqa,pab->pqb", as_float(block_half[second_ids]), pair_maps[:, 1], precision=highest).astype(jnp.bfloat16)
            left_parts = as_float(first_proj).reshape(PAIR_GRP, N_ORB, slice_rows, P_SIZE)
            right_parts = as_float(second_proj).reshape(PAIR_GRP, N_ORB, slice_rows, P_SIZE)
            partial_value = jnp.einsum("psqa,psqb->psab", left_parts, right_parts, precision=highest)
            integrals = jnp.sum(as_float(partial_value.astype(jnp.bfloat16)), axis=1)
            partner_ids = lax.dynamic_slice_in_dim(couple, first_row, PAIR_GRP)
            partners = as_float(amp_half[partner_ids])
            intersection = as_float(lax.dynamic_slice_in_dim(couple_intersection, first_row, PAIR_GRP))
            half_products = jnp.einsum("pkab,pkbc->pkac", intersection, partners, precision=highest).astype(jnp.bfloat16)
            coupled = jnp.einsum("pkac,pkdc->pad", as_float(half_products), intersection, precision=highest)
            own_amps = as_float(lax.dynamic_slice_in_dim(amp_half, first_row, PAIR_GRP))
            fitted_half = jnp.einsum("pqa,pab->pqb", as_float(second_proj), own_amps, precision=highest).astype(jnp.bfloat16)
            returned = jnp.einsum("pqb,pcb->pqc", as_float(fitted_half), pair_maps[:, 0], precision=highest)
            fitted = fitted.at[first_ids].add(returned)
            return fitted, integrals + coupled

        start_fitted = jnp.zeros((NORB, Q, P_SIZE), jnp.float32)
        fitted, driving = lax.scan(one_block, start_fitted, jnp.arange(block_total, dtype=jnp.int32))
        driving = driving.reshape(NPAIR, P_SIZE, P_SIZE)
        dressed = bare_blocks + dress_scale * fitted
        amps_now = -driving / denominator
    return amps_now, dressed
```

```python
import functools

import jax
import jax.numpy as jnp
from jax import lax
from jax.experimental import pallas as pl
from jax.experimental.pallas import tpu as pltpu
from jax.sharding import PartitionSpec as P

REACH = 1
ITERS = 2
SIDES = 2 * REACH + 1

dress_scale = 0.015

NN = (((1,), (0,)), ((), ()))
NT = (((1,), (1,)), ((), ()))


def dot(left, right, dims=NN):
    return lax.dot_general(left, right, dims, preferred_element_type=jnp.float32)


def kernel(
    ranks,
    groups,
    couple_hbm,
    first_hbm,
    second_hbm,
    energy_hbm,
    amps_hbm,
    pno_hbm,
    inter_hbm,
    maps_hbm,
    orb_hbm,
    out_amps,
    out_dressed,
    couple,
    occ_first,
    occ_second,
    occ_energy,
    second_at,
    amplitudes,
    pno_energy,
    inter,
    maps,
    first_t,
    blocks_t,
    scale,
    coupled,
    amps_0,
    amps_1,
    window_0,
    window_1,
    parts_out,
    parts_in,
    half,
    fitted,
    amp_send,
    amp_recv,
    win_send,
    win_recv,
    part_send,
    part_recv,
    inter_sem,
    maps_sem,
    orb_sem,
    small_sem,
):
    amps = (amps_0, amps_1)
    window = (window_0, window_1)
    own_pairs = amps_hbm.shape[0]
    orbs = orb_hbm.shape[0]
    partners = couple.shape[1]
    size = amplitudes.shape[2]
    virtuals = orb_hbm.shape[2]
    pairs = ranks * own_pairs
    me = lax.axis_index("orb")
    group = lax.axis_index("pair")
    own = me * own_pairs
    middle = pl.ds(REACH * orbs, orbs)
    places = [place for place in range(SIDES) if place != REACH]
    bf16 = jnp.bfloat16
    square = ranks == 4
    steps = (3, 1, 2) if square else tuple(range(1, ranks))

    def target(step):
        if square:
            return (me // 2 + step // 2) % 2 * 2 + (me + step) % 2
        return (me + step) % ranks

    def source(step):
        return target(step) if square else (me + ranks - step) % ranks

    barrier = pltpu.get_barrier_semaphore()
    for step in range(1, ranks):
        pl.semaphore_signal(
            barrier,
            inc=1,
            device_id={"orb": (me + step) % ranks},
            device_id_type=pl.DeviceIdType.MESH,
        )
    for step in range(1, REACH + 1):
        for shift in (step, groups - step):
            pl.semaphore_signal(
                barrier,
                inc=1,
                device_id={"pair": (group + shift) % groups},
                device_id_type=pl.DeviceIdType.MESH,
            )

    orb_copy = pltpu.make_async_copy(orb_hbm, window[0].at[middle], orb_sem)
    orb_copy.start()
    small_copies = [
        pltpu.make_async_copy(source_ref, target_ref, small_sem.at[at])
        for at, (source_ref, target_ref) in enumerate(
            (
                (amps_hbm, amplitudes),
                (first_hbm, occ_first),
                (second_hbm, occ_second),
                (energy_hbm, occ_energy),
                (pno_hbm, pno_energy),
                (couple_hbm, couple),
            )
        )
    ]
    for copy in small_copies:
        copy.start()
    maps_copy = pltpu.make_async_copy(maps_hbm, maps, maps_sem)
    maps_copy.start()
    inter_copy = pltpu.make_async_copy(inter_hbm, inter, inter_sem)
    inter_copy.start()

    small_copies[0].wait()
    for i in range(own_pairs):
        amps[0][own + i] = amplitudes[i].astype(bf16)
    orb_copy.wait()
    pl.semaphore_wait(barrier, ranks - 1 + 2 * REACH)

    def win_copy(turn, place):
        return pltpu.make_async_remote_copy(
            src_ref=window[turn].at[middle],
            dst_ref=window[turn].at[pl.ds(place * orbs, orbs)],
            send_sem=win_send.at[turn],
            recv_sem=win_recv.at[turn, place],
            device_id={"pair": (group + REACH - place + groups) % groups},
            device_id_type=pl.DeviceIdType.MESH,
        )

    def amp_copy(turn, step, i):
        return pltpu.make_async_remote_copy(
            src_ref=amps[turn].at[own + i],
            dst_ref=amps[turn].at[own + i],
            send_sem=amp_send.at[turn],
            recv_sem=amp_recv.at[turn, step],
            device_id={"orb": target(step)},
            device_id_type=pl.DeviceIdType.MESH,
        )

    def part_copy(turn, step, i):
        return pltpu.make_async_remote_copy(
            src_ref=parts_out.at[turn, i, step],
            dst_ref=parts_in.at[turn, i, step - 1],
            send_sem=part_send.at[turn],
            recv_sem=part_recv.at[turn, i],
            device_id={"orb": target(step)},
            device_id_type=pl.DeviceIdType.MESH,
        )

    def whole(ref, send_sem, recv_sem):
        return pltpu.make_async_remote_copy(
            src_ref=ref,
            dst_ref=ref,
            send_sem=send_sem,
            recv_sem=recv_sem,
            device_id={"orb": target(1)},
            device_id_type=pl.DeviceIdType.MESH,
        )

    def amp_wait(turn, step):
        block = amps[turn].at[pl.ds(source(step) * own_pairs, own_pairs)]
        whole(block, amp_send.at[turn], amp_recv.at[turn, step]).wait_recv()

    def part_wait(turn, i):
        whole(parts_in.at[turn, i], part_send.at[turn], part_recv.at[turn, i]).wait_recv()

    def sent(turn):
        sends = pl.ds(0, (ranks - 1) * own_pairs)
        whole(amps[turn].at[sends], amp_send.at[turn], amp_recv.at[turn, 0]).wait_send()
        sends = pl.ds(0, len(places) * orbs)
        whole(window[turn].at[sends], win_send.at[turn], win_recv.at[turn, 0]).wait_send()

    def parts_sent(turn):
        whole(parts_in.at[turn], part_send.at[turn], part_recv.at[turn, 0]).wait_send()

    def amp_start(turn, i):
        for step in steps:
            amp_copy(turn, step, i).start()

    def win_start(turn):
        for place in places:
            win_copy(turn, place).start()

    def transposed(turn):
        for o in range(orbs):
            blocks_t[o] = window[turn][REACH * orbs + o].T

    def integrals(turn):
        for place in places:
            win_copy(turn, place).wait_recv()

        def one(i):
            for step in steps + (0,):
                pair = target(step) * own_pairs + i
                left = blocks_t[occ_first[pair] % orbs]
                parts_out[turn, i, step] = dot(left, window[turn][second_at[pair]]).astype(bf16)
                if step > 0:
                    part_copy(turn, step, i).start()

        if square:
            for i in range(own_pairs):
                one(i)
        else:
            pl.loop(0, own_pairs)(one)

    def fit(turn, base):
        lefts, rights = [], []
        for i in range(own_pairs):
            pair = base + i
            half_way = dot(maps[pair, 1], amps[turn][pair]).astype(bf16)
            through = dot(half_way, maps[pair, 0], NT)
            local = occ_first[pair] % orbs
            rights.append(
                jnp.concatenate(
                    [jnp.where(local == o, through, 0.0).astype(bf16) for o in range(orbs)], axis=1
                )
            )
            lefts.append(window[turn][second_at[pair]])
        return dot(jnp.concatenate(lefts, axis=1), jnp.concatenate(rights, axis=0))

    def fit_all(turn):
        fitted[...] = fit(turn, own)

        @pl.loop(1, ranks)
        def _(step):
            amp_wait(turn, step)
            fitted[...] += fit(turn, source(step) * own_pairs)

    def dress(turn):
        for o in range(orbs):
            value = window[0][REACH * orbs + o].astype(jnp.float32)
            value += dress_scale * fitted[:, o * virtuals : (o + 1) * virtuals]
            if turn + 1 < ITERS:
                window[turn + 1][REACH * orbs + o] = value.astype(bf16)
            else:
                out_dressed[o] = value

    def couplings(turn, i):
        for k in range(partners):
            partner = couple[i, k] % pairs
            half[:, k * size : (k + 1) * size] = dot(inter[i, k], amps[turn][partner]).astype(bf16)
        total = None
        for k in range(0, partners, 2):
            right = jnp.concatenate([inter[i, k], inter[i, k + 1]], axis=1)
            term = dot(half[:, k * size : (k + 2) * size], right, NT)
            total = term if total is None else total + term
        coupled[i] = total

    def finish(turn, i):
        part_wait(turn, i)
        total = parts_out[turn, i, 0].astype(jnp.float32)
        for step in range(1, ranks):
            total += parts_in[turn, i, step - 1].astype(jnp.float32)
        right = dot(total.astype(bf16), maps[own + i, 1]).astype(bf16)
        value = (dot(first_t[i], right) + coupled[i]) * scale[i]
        if turn + 1 < ITERS:
            amps[turn + 1][own + i] = value.astype(bf16)
            amp_start(turn + 1, i)
        else:
            out_amps[i] = value

    win_start(0)
    for i in range(own_pairs):
        amp_start(0, i)

    for copy in small_copies[1:]:
        copy.wait()

    @pl.loop(0, pairs)
    def _(pair):
        second = occ_second[pair]
        distance = (second // orbs - group + REACH + groups) % groups
        second_at[pair] = jnp.minimum(distance, SIDES - 1) * orbs + second % orbs

    transposed(0)
    maps_copy.wait()
    for i in range(own_pairs):
        first_t[i] = maps[own + i, 0].T
        rows = jnp.broadcast_to(pno_energy[pl.ds(i, 1), :], (size, size))
        denominator = rows + rows.T
        denominator -= occ_energy[occ_first[own + i]]
        denominator -= occ_energy[occ_second[own + i]]
        scale[i] = -1.0 / denominator

    for turn in range(ITERS):
        last = turn + 1 == ITERS
        integrals(turn)
        fit_all(turn)
        dress(turn)
        if not last:
            win_start(turn + 1)
            transposed(turn + 1)
        if turn == 0:
            inter_copy.wait()
        for i in range(own_pairs):
            couplings(turn, i)
        if last:
            sent(turn - 1)
            parts_sent(turn - 1)
        for i in range(own_pairs):
            finish(turn, i)

    sent(ITERS - 1)
    parts_sent(ITERS - 1)


def store(amps, dressed, out_amps, out_dressed, sem):
    copies = [
        pltpu.make_async_copy(amps, out_amps, sem.at[0]),
        pltpu.make_async_copy(dressed, out_dressed, sem.at[1]),
    ]
    for copy in copies:
        copy.start()
    for copy in copies:
        copy.wait()


def on_device(
    ranks,
    groups,
    amplitudes,
    couple,
    occ_first,
    occ_second,
    couple_intersection,
    pno_maps,
    orbital_blocks,
    pno_energy,
    occ_energy,
):
    own_pairs, size, _ = amplitudes.shape
    group_pairs = occ_first.shape[0]
    orbs, rows, virtuals = orbital_blocks.shape
    partners = couple.shape[1]
    bf16 = jnp.bfloat16
    vmem = pl.BlockSpec(memory_space=pltpu.VMEM)
    hbm = pl.BlockSpec(memory_space=pltpu.HBM)
    dma = pltpu.SemaphoreType.DMA
    results = pl.pallas_call(
        functools.partial(kernel, ranks, groups),
        out_shape=(
            pltpu.VMEM(amplitudes.shape, jnp.float32),
            pltpu.VMEM(orbital_blocks.shape, jnp.float32),
        ),
        in_specs=[hbm] * 9,
        out_specs=(vmem, vmem),
        scratch_shapes=[
            pltpu.SMEM(couple.shape, couple.dtype),
            pltpu.SMEM(occ_first.shape, occ_first.dtype),
            pltpu.SMEM(occ_second.shape, occ_second.dtype),
            pltpu.SMEM(occ_energy.shape, occ_energy.dtype),
            pltpu.SMEM(occ_second.shape, occ_second.dtype),
            pltpu.VMEM(amplitudes.shape, amplitudes.dtype),
            pltpu.VMEM(pno_energy.shape, pno_energy.dtype),
            pltpu.VMEM(couple_intersection.shape, bf16),
            pltpu.VMEM(pno_maps.shape, bf16),
            pltpu.VMEM((own_pairs, size, virtuals), bf16),
            pltpu.VMEM((orbs, virtuals, rows), bf16),
            pltpu.VMEM((own_pairs, size, size), jnp.float32),
            pltpu.VMEM((own_pairs, size, size), jnp.float32),
            pltpu.VMEM((group_pairs, size, size), bf16),
            pltpu.VMEM((group_pairs, size, size), bf16),
            pltpu.VMEM((SIDES * orbs, rows, virtuals), bf16),
            pltpu.VMEM((SIDES * orbs, rows, virtuals), bf16),
            pltpu.VMEM((ITERS, own_pairs, ranks, virtuals, virtuals), bf16),
            pltpu.VMEM((ITERS, own_pairs, ranks - 1, virtuals, virtuals), bf16),
            pltpu.VMEM((size, partners * size), bf16),
            pltpu.VMEM((rows, orbs * virtuals), jnp.float32),
            dma((ITERS,)),
            dma((ITERS, ranks)),
            dma((ITERS,)),
            dma((ITERS, SIDES)),
            dma((ITERS,)),
            dma((ITERS, own_pairs)),
            dma,
            dma,
            dma,
            dma((6,)),
        ],
        compiler_params=pltpu.CompilerParams(
            collective_id=0, has_side_effects=True, vmem_limit_bytes=67043328 - 4096 * 1024
        ),
    )(
        *(pltpu.with_memory_space_constraint(x, pltpu.HBM) for x in (
        couple,
        occ_first,
        occ_second,
        occ_energy,
        amplitudes,
        pno_energy,
        couple_intersection,
        pno_maps,
        orbital_blocks,
        ))
    )
    return pl.pallas_call(
        store,
        out_shape=tuple(pltpu.HBM(x.shape, x.dtype) for x in results),
        in_specs=[vmem] * 2,
        out_specs=(hbm, hbm),
        scratch_shapes=[dma((2,))],
        compiler_params=pltpu.CompilerParams(vmem_limit_bytes=4096 * 1024),
    )(*(pltpu.with_memory_space_constraint(x, pltpu.VMEM) for x in results))


def solution(mesh):
    return jax.shard_map(
        functools.partial(on_device, mesh.shape["orb"], mesh.shape["pair"]),
        mesh=mesh,
        in_specs=(
            P(("pair", "orb"), None, None),
            P(("pair", "orb"), None),
            P("pair"),
            P("pair"),
            P(("pair", "orb"), None, None, None),
            P("pair", None, None, None),
            P("pair", "orb", None),
            P(("pair", "orb"), None),
            P(),
        ),
        out_specs=(P(("pair", "orb"), None, None), P("pair", "orb", None)),
        check_vma=False,
    )
```

```python
import functools

import jax
import jax.numpy as jnp
from jax import lax
from jax.experimental import pallas as pl
from jax.experimental.pallas import tpu as pltpu
from jax.sharding import PartitionSpec as P

REACH = 1
ITERS = 2
SIDES = 2 * REACH + 1

dress_scale = 0.015
BATCH = 2

NN = (((1,), (0,)), ((), ()))
NT = (((1,), (1,)), ((), ()))


def dot(left, right, dims=NN):
    return lax.dot_general(left, right, dims, preferred_element_type=jnp.float32)


def kernel(
    ranks,
    groups,
    couple_hbm,
    first_hbm,
    second_hbm,
    energy_hbm,
    amps_hbm,
    pno_hbm,
    inter_hbm,
    maps_hbm,
    orb_hbm,
    out_amps,
    out_dressed,
    couple,
    occ_first,
    occ_second,
    occ_energy,
    second_at,
    amplitudes,
    pno_energy,
    inter,
    inter_t,
    maps,
    first_t,
    blocks_t,
    scale,
    coupled,
    amps,
    amps_now,
    window,
    blocks,
    parts_out,
    parts_in,
    relayed,
    weights,
    fitted,
    amp_send,
    amp_recv,
    win_send,
    win_recv,
    part_send,
    part_recv,
    relay_recv,
    inter_sem,
    maps_sem,
    orb_sem,
    small_sem,
):
    own_pairs = amps_hbm.shape[0]
    orbs = orb_hbm.shape[0]
    partners = couple.shape[1]
    size = amplitudes.shape[2]
    virtuals = orb_hbm.shape[2]
    pairs = ranks * own_pairs
    me = lax.axis_index("orb")
    group = lax.axis_index("pair")
    own = me * own_pairs
    middle = pl.ds(REACH * orbs, orbs)
    places = [place for place in range(SIDES) if place != REACH]
    bf16 = jnp.bfloat16
    square = ranks == 4 and own_pairs % 2 == 0
    z_place = (group + 1) % 2 * 2 * REACH
    c_place = 2 * REACH - z_place

    def target(step):
        if square:
            return (me // 2 + step // 2) % 2 * 2 + (me + step) % 2
        return (me + step) % ranks

    def source(step):
        return target(step) if square else (me + ranks - step) % ranks

    barrier = pltpu.get_barrier_semaphore()
    for step in range(1, ranks):
        pl.semaphore_signal(
            barrier,
            inc=1,
            device_id={"orb": (me + step) % ranks},
            device_id_type=pl.DeviceIdType.MESH,
        )
    for step in range(1, REACH + 1):
        for shift in (step, groups - step):
            pl.semaphore_signal(
                barrier,
                inc=1,
                device_id={"pair": (group + shift) % groups},
                device_id_type=pl.DeviceIdType.MESH,
            )

    small_copies = [
        pltpu.make_async_copy(source_ref, target_ref, small_sem.at[at])
        for at, (source_ref, target_ref) in enumerate(
            (
                (amps_hbm, amplitudes),
                (first_hbm, occ_first),
                (second_hbm, occ_second),
                (energy_hbm, occ_energy),
                (pno_hbm, pno_energy),
                (couple_hbm, couple),
            )
        )
    ]
    small_copies[0].start()
    pl.semaphore_wait(barrier, ranks - 1 + 2 * REACH)

    def win_copy(turn, place, bare=False):
        return pltpu.make_async_remote_copy(
            src_ref=orb_hbm if bare else window.at[turn, middle],
            dst_ref=window.at[turn, pl.ds(place * orbs, orbs)],
            send_sem=win_send.at[turn],
            recv_sem=win_recv.at[turn, place],
            device_id={"pair": (group + REACH - place + groups) % groups},
            device_id_type=pl.DeviceIdType.MESH,
        )

    def amp_copy(turn, step, i):
        return pltpu.make_async_remote_copy(
            src_ref=amps.at[turn, own + i],
            dst_ref=amps.at[turn, own + i],
            send_sem=amp_send.at[turn],
            recv_sem=amp_recv.at[turn, step, i],
            device_id={"orb": target(step)},
            device_id_type=pl.DeviceIdType.MESH,
        )

    def amp_relay(turn, i):
        via, onto = (1, 2) if i % 2 == 0 else (2, 1)
        place = target(via) * own_pairs + i
        return pltpu.make_async_remote_copy(
            src_ref=amps.at[turn, place],
            dst_ref=amps.at[turn, place],
            send_sem=amp_send.at[turn],
            recv_sem=amp_recv.at[turn, 3, i],
            device_id={"orb": target(onto)},
            device_id_type=pl.DeviceIdType.MESH,
        )

    def relay_all(turn):
        for i in range(own_pairs):
            amp_copy(turn, 1 if i % 2 == 0 else 2, i).wait_recv()
            amp_relay(turn, i).start()

    def amp_wait(turn, step):
        for i in range(own_pairs):
            def wait(i=i):
                amp_copy(turn, step, i).wait_recv()

            if not square or step == 3 or (step, i % 2) in ((1, 1), (2, 0)):
                wait()

    def part_copy(turn, step, i):
        return pltpu.make_async_remote_copy(
            src_ref=parts_out.at[turn, i, step],
            dst_ref=parts_in.at[turn, i, step - 1],
            send_sem=part_send.at[turn],
            recv_sem=part_recv.at[turn, i],
            device_id={"orb": target(step)},
            device_id_type=pl.DeviceIdType.MESH,
        )

    def part_relay(turn, i):
        return pltpu.make_async_remote_copy(
            src_ref=parts_out.at[turn, i, 3],
            dst_ref=relayed.at[turn, i],
            send_sem=part_send.at[turn],
            recv_sem=relay_recv.at[turn, i],
            device_id={"orb": target(1 if i % 2 == 0 else 2)},
            device_id_type=pl.DeviceIdType.MESH,
        )

    def forward_all(turn):
        for i in range(own_pairs):
            onto = 2 if i % 2 == 0 else 1
            part_relay(turn, i).wait_recv()
            total = parts_out[turn, i, onto].astype(jnp.float32)
            total += relayed[turn, i].astype(jnp.float32)
            parts_out[turn, i, onto] = total.astype(bf16)
            part_copy(turn, onto, i).start()

    def whole(ref, send_sem, recv_sem):
        return pltpu.make_async_remote_copy(
            src_ref=ref,
            dst_ref=ref,
            send_sem=send_sem,
            recv_sem=recv_sem,
            device_id={"orb": target(1)},
            device_id_type=pl.DeviceIdType.MESH,
        )

    def part_wait(turn, i):
        def wait(terms):
            arrived = parts_in.at[turn, i, pl.ds(0, terms)]
            whole(arrived, part_send.at[turn], part_recv.at[turn, i]).wait_recv()

        wait(2 if square else ranks - 1)

    def sent(turn):
        sends = pl.ds(0, (ranks - 1) * own_pairs)
        whole(amps.at[turn, sends], amp_send.at[turn], amp_recv.at[turn, 0, 0]).wait_send()
        sends = pl.ds(0, len(places) * orbs)
        whole(window.at[turn, sends], win_send.at[turn], win_recv.at[turn, 0]).wait_send()

    def parts_sent(turn):
        whole(parts_in.at[turn], part_send.at[turn], part_recv.at[turn, 0]).wait_send()

    def amp_start(turn, i):
        for step in (1, 2) if square else range(ranks - 1, 0, -1):
            amp_copy(turn, step, i).start()

    def win_start(turn, bare=False):
        win_copy(turn, z_place, bare).start()
        win_copy(turn, c_place, bare).start()

    def transposed(turn):
        for o in range(orbs):
            blocks_t[o] = window[turn, REACH * orbs + o].T

    def integral(turn, step, i):
        pair = target(step) * own_pairs + i
        left = blocks_t[occ_first[pair] % orbs]
        parts_out[turn, i, step] = dot(left, blocks[second_at[pair]]).astype(bf16)

    def integrals(turn):
        for place in places:
            win_copy(turn, place).wait_recv()
        for at in range(SIDES * orbs):
            blocks[at] = window[turn, at]

        def one(i):
            for step in range(ranks - 1, -1, -1):
                integral(turn, step, i)
                if step > 0 and not square:
                    part_copy(turn, step, i).start()

        if square:
            for i in range(own_pairs):
                integral(turn, 3, i)
            for i in range(own_pairs):
                for step in (2, 1, 0):
                    integral(turn, step, i)
        else:
            pl.loop(0, own_pairs)(one)

    def far_sums(turn):
        for i in range(own_pairs):
            part_relay(turn, i).start()

    def near_sums(turn):
        for i in range(own_pairs):
            part_copy(turn, 1 if i % 2 == 0 else 2, i).start()

    def through(turn, step):
        base = source(step) * own_pairs
        halves = []
        for i in range(own_pairs):
            amp = amps[turn, base + i]
            amps_now[base + i] = amp
            halves.append(dot(maps[base + i, 1], amp).astype(bf16))
        wholes = [dot(halves[i], first_t[base + i]) for i in range(own_pairs)]
        for i in range(own_pairs):
            local = occ_first[base + i] % orbs
            rows = pl.ds((step * own_pairs + i) * virtuals, virtuals)
            for o in range(orbs):
                masked = jnp.where(local == o, wholes[i], 0.0).astype(bf16)
                weights[rows, o * virtuals : (o + 1) * virtuals] = masked

    def applied(turn, some):
        lefts = [
            blocks[second_at[source(step) * own_pairs + i]]
            for step in some
            for i in range(own_pairs)
        ]
        rows = own_pairs * virtuals
        right = weights[pl.ds(some[0] * rows, len(some) * rows), :]
        return dot(jnp.concatenate(lefts, axis=1), right)

    def fit_near(turn):
        fitted[...] = applied(turn, near_steps)

    def dress(turn):
        if square:
            total = fitted[...] + applied(turn, far_steps)
        else:

            @pl.loop(1, ranks)
            def _(step):
                fitted[...] += applied(turn, (step,))

            total = fitted[...]
        values = [
            window[0, REACH * orbs + o].astype(jnp.float32)
            + dress_scale * total[:, o * virtuals : (o + 1) * virtuals]
            for o in range(orbs)
        ]

        @pl.when(turn + 1 < ITERS)
        def _():
            for o in range(orbs):
                window[turn + 1, REACH * orbs + o] = values[o].astype(bf16)

        @pl.when(turn + 1 == ITERS)
        def _():
            for o in range(orbs):
                out_dressed[o] = values[o]

    def couplings(turn):
        def one(i):
            halves = [
                dot(inter[i, k], amps_now[couple[i, k] % pairs]).astype(bf16)
                for k in range(partners)
            ]
            coupled[i] = dot(jnp.concatenate(halves, axis=1), inter_t[i])

        for i in range(own_pairs):
            one(i)

    def finish(turn):
        for first in range(0, own_pairs, BATCH):
            batch = range(first, min(first + BATCH, own_pairs))
            for i in batch:
                part_wait(turn, i)
            totals = {}
            for i in batch:
                total = parts_out[turn, i, 0].astype(jnp.float32)
                for step in range(1, 3 if square else ranks):
                    total += parts_in[turn, i, step - 1].astype(jnp.float32)
                totals[i] = total.astype(bf16)
            rights = {i: dot(totals[i], maps[own + i, 1]).astype(bf16) for i in batch}
            values = {
                i: (dot(first_t[own + i], rights[i]) + coupled[i]) * scale[i] for i in batch
            }

            @pl.when(turn + 1 < ITERS)
            def _(batch=batch, values=values):
                for i in batch:
                    amps[turn + 1, own + i] = values[i].astype(bf16)
                    amp_start(turn + 1, i)

            @pl.when(turn + 1 == ITERS)
            def _(batch=batch, values=values):
                for i in batch:
                    out_amps[i] = values[i]

    win_start(0, True)
    orb_copy = pltpu.make_async_copy(orb_hbm, window.at[0, middle], orb_sem)
    orb_copy.start()
    small_copies[0].wait()
    for i in range(own_pairs):
        amps[0, own + i] = amplitudes[i].astype(bf16)
    for i in range(own_pairs):
        amp_start(0, i)
    for copy in small_copies[1:]:
        copy.start()
    maps_copy = pltpu.make_async_copy(maps_hbm, maps, maps_sem)
    maps_copy.start()
    inter_copy = pltpu.make_async_copy(inter_hbm, inter, inter_sem)
    inter_copy.start()

    for copy in small_copies[1:]:
        copy.wait()

    @pl.loop(0, pairs)
    def _(pair):
        second = occ_second[pair]
        distance = (second // orbs - group + REACH + groups) % groups
        second_at[pair] = jnp.minimum(distance, SIDES - 1) * orbs + second % orbs

    orb_copy.wait()
    transposed(0)
    maps_copy.wait()

    @pl.loop(0, ranks)
    def _(block):
        for i in range(own_pairs):
            first_t[block * own_pairs + i] = maps[block * own_pairs + i, 0].T

    inter_copy.wait()

    @pl.loop(0, own_pairs)
    def _(i):
        rows = jnp.broadcast_to(pno_energy[pl.ds(i, 1), :], (size, size))
        denominator = rows + rows.T
        denominator -= occ_energy[occ_first[own + i]]
        denominator -= occ_energy[occ_second[own + i]]
        scale[i] = -1.0 / denominator
        for k in range(partners):
            inter_t[i, k * size : (k + 1) * size, :] = inter[i, k].T

    near_steps = (0, 1, 2) if square else (0,)
    far_steps = (3,) if square else tuple(range(1, ranks))

    def throughs(turn, some):
        if square:
            for step in some:
                if step > 0:
                    amp_wait(turn, step)
        first, last = some[0], some[-1] + 1

        @pl.loop(first, last)
        def _(step):
            if not square and first > 0:
                amp_wait(turn, step)
            through(turn, step)

    near_steps = (0, 1, 2) if square else (0,)
    far_steps = (3,) if square else tuple(range(1, ranks))
    inner = group % 2 == 1

    throughs(0, (0,))
    if square:
        relay_all(0)

    @pl.loop(0, ITERS)
    def _(turn):
        integrals(turn)

        if square:

            @pl.when(turn == 0)
            def _():
                far_sums(turn)

            @pl.when(turn > 0)
            def _():
                @pl.when(jnp.logical_not(inner))
                def _():
                    far_sums(turn)

                throughs(turn, (0,))
                relay_all(turn)

                @pl.when(jnp.logical_not(inner))
                def _():
                    near_sums(turn)

            throughs(turn, (1, 2))
        else:

            @pl.when(turn > 0)
            def _():
                throughs(turn, (0,))

        fit_near(turn)
        if square:

            @pl.when(turn > 0)
            def _():
                @pl.when(inner)
                def _():
                    far_sums(turn)
                    near_sums(turn)

                forward_all(turn)

        throughs(turn, far_steps)
        dress(turn)

        @pl.when(turn + 1 < ITERS)
        def _():
            win_start(turn + 1)
            if square:
                near_sums(turn)
                forward_all(turn)
            transposed(turn + 1)

        couplings(turn)

        @pl.when(turn > 0)
        def _():
            sent(turn - 1)
            parts_sent(turn - 1)

        finish(turn)

    sent(ITERS - 1)
    parts_sent(ITERS - 1)


def store(amps, dressed, out_amps, out_dressed, sem):
    copies = [
        pltpu.make_async_copy(amps, out_amps, sem.at[0]),
        pltpu.make_async_copy(dressed, out_dressed, sem.at[1]),
    ]
    for copy in copies:
        copy.start()
    for copy in copies:
        copy.wait()


def on_device(
    ranks,
    groups,
    amplitudes,
    couple,
    occ_first,
    occ_second,
    couple_intersection,
    pno_maps,
    orbital_blocks,
    pno_energy,
    occ_energy,
):
    own_pairs, size, _ = amplitudes.shape
    group_pairs = occ_first.shape[0]
    orbs, rows, virtuals = orbital_blocks.shape
    partners = couple.shape[1]
    bf16 = jnp.bfloat16
    vmem = pl.BlockSpec(memory_space=pltpu.VMEM)
    hbm = pl.BlockSpec(memory_space=pltpu.HBM)
    dma = pltpu.SemaphoreType.DMA
    results = pl.pallas_call(
        functools.partial(kernel, ranks, groups),
        out_shape=(
            pltpu.VMEM(amplitudes.shape, jnp.float32),
            pltpu.VMEM(orbital_blocks.shape, jnp.float32),
        ),
        in_specs=[hbm] * 9,
        out_specs=(vmem, vmem),
        scratch_shapes=[
            pltpu.SMEM(couple.shape, couple.dtype),
            pltpu.SMEM(occ_first.shape, occ_first.dtype),
            pltpu.SMEM(occ_second.shape, occ_second.dtype),
            pltpu.SMEM(occ_energy.shape, occ_energy.dtype),
            pltpu.SMEM(occ_second.shape, occ_second.dtype),
            pltpu.VMEM(amplitudes.shape, amplitudes.dtype),
            pltpu.VMEM(pno_energy.shape, pno_energy.dtype),
            pltpu.VMEM(couple_intersection.shape, bf16),
            pltpu.VMEM((own_pairs, partners * size, size), bf16),
            pltpu.VMEM(pno_maps.shape, bf16),
            pltpu.VMEM((group_pairs, size, virtuals), bf16),
            pltpu.VMEM((orbs, virtuals, rows), bf16),
            pltpu.VMEM((own_pairs, size, size), jnp.float32),
            pltpu.VMEM((own_pairs, size, size), jnp.float32),
            pltpu.VMEM((ITERS, group_pairs, size, size), bf16),
            pltpu.VMEM((group_pairs, size, size), bf16),
            pltpu.VMEM((ITERS, SIDES * orbs, rows, virtuals), bf16),
            pltpu.VMEM((SIDES * orbs, rows, virtuals), bf16),
            pltpu.VMEM((ITERS, own_pairs, ranks, virtuals, virtuals), bf16),
            pltpu.VMEM((ITERS, own_pairs, ranks - 1, virtuals, virtuals), bf16),
            pltpu.VMEM((ITERS, own_pairs, virtuals, virtuals), bf16),
            pltpu.VMEM((group_pairs * virtuals, orbs * virtuals), bf16),
            pltpu.VMEM((rows, orbs * virtuals), jnp.float32),
            dma((ITERS,)),
            dma((ITERS, ranks, own_pairs)),
            dma((ITERS,)),
            dma((ITERS, SIDES)),
            dma((ITERS,)),
            dma((ITERS, own_pairs)),
            dma((ITERS, own_pairs)),
            dma,
            dma,
            dma,
            dma((6,)),
        ],
        compiler_params=pltpu.CompilerParams(
            collective_id=0, has_side_effects=True, vmem_limit_bytes=67043328 - 4096 * 1024
        ),
    )(
        *(pltpu.with_memory_space_constraint(x, pltpu.HBM) for x in (
        couple,
        occ_first,
        occ_second,
        occ_energy,
        amplitudes,
        pno_energy,
        couple_intersection,
        pno_maps,
        orbital_blocks,
        ))
    )
    return pl.pallas_call(
        store,
        out_shape=tuple(pltpu.HBM(x.shape, x.dtype) for x in results),
        in_specs=[vmem] * 2,
        out_specs=(hbm, hbm),
        scratch_shapes=[dma((2,))],
        compiler_params=pltpu.CompilerParams(vmem_limit_bytes=4096 * 1024),
    )(*(pltpu.with_memory_space_constraint(x, pltpu.VMEM) for x in results))


def solution(mesh):
    return jax.shard_map(
        functools.partial(on_device, mesh.shape["orb"], mesh.shape["pair"]),
        mesh=mesh,
        in_specs=(
            P(("pair", "orb"), None, None),
            P(("pair", "orb"), None),
            P("pair"),
            P("pair"),
            P(("pair", "orb"), None, None, None),
            P("pair", None, None, None),
            P("pair", "orb", None),
            P(("pair", "orb"), None),
            P(),
        ),
        out_specs=(P(("pair", "orb"), None, None), P("pair", "orb", None)),
        check_vma=False,
    )
```

```python
import functools

import jax
import jax.numpy as jnp
from jax import lax
from jax.experimental import pallas as pl
from jax.experimental.pallas import tpu as pltpu
from jax.sharding import PartitionSpec as P

REACH = 1
ITERS = 2
SIDES = 2 * REACH + 1

dress_scale = 0.015
BATCH = 2
GATHER_DIRECT = ("none", "none")
SUM_DIRECT = ("outer", "none")
NONE = ("none", "none")
FIRST_RELAY = "all"
INNER_FAR = 1
INNER_NEAR = 2

NN = (((1,), (0,)), ((), ()))
NT = (((1,), (1,)), ((), ()))


def dot(left, right, dims=NN):
    return lax.dot_general(left, right, dims, preferred_element_type=jnp.float32)


def kernel(
    ranks,
    groups,
    couple_hbm,
    first_hbm,
    second_hbm,
    energy_hbm,
    amps_hbm,
    pno_hbm,
    inter_hbm,
    maps_hbm,
    orb_hbm,
    out_amps,
    out_dressed,
    couple,
    occ_first,
    occ_second,
    occ_energy,
    second_at,
    amplitudes,
    pno_energy,
    inter,
    inter_t,
    maps,
    first_t,
    blocks_t,
    scale,
    coupled,
    amps,
    amps_now,
    window,
    blocks,
    parts_out,
    parts_in,
    relayed,
    weights,
    fitted,
    amp_send,
    amp_recv,
    win_send,
    win_recv,
    part_send,
    part_recv,
    relay_recv,
    inter_sem,
    maps_sem,
    orb_sem,
    small_sem,
):
    own_pairs = amps_hbm.shape[0]
    orbs = orb_hbm.shape[0]
    partners = couple.shape[1]
    size = amplitudes.shape[2]
    virtuals = orb_hbm.shape[2]
    pairs = ranks * own_pairs
    me = lax.axis_index("orb")
    group = lax.axis_index("pair")
    own = me * own_pairs
    middle = pl.ds(REACH * orbs, orbs)
    places = [place for place in range(SIDES) if place != REACH]
    bf16 = jnp.bfloat16
    square = ranks == 4 and own_pairs % 2 == 0
    z_place = (group + 1) % 2 * 2 * REACH
    c_place = 2 * REACH - z_place

    def target(step):
        if square:
            return (me // 2 + step // 2) % 2 * 2 + (me + step) % 2
        return (me + step) % ranks

    def source(step):
        return target(step) if square else (me + ranks - step) % ranks

    inner = group % 2 == 1

    def kinds(modes, turn):
        flags = [{"none": False, "all": True, "outer": jnp.logical_not(inner)}[m] for m in modes]
        if isinstance(turn, int):
            return flags[turn]
        if all(mode == modes[0] for mode in modes):
            return flags[0]
        flag = False
        for at in range(ITERS):
            flag = jnp.logical_or(flag, jnp.logical_and(turn == at, flags[at]))
        return flag

    def either(flag, yes, no):
        if isinstance(flag, bool):
            (yes if flag else no)()
        else:
            pl.when(flag)(yes)
            pl.when(jnp.logical_not(flag))(no)

    def nothing():
        pass

    barrier = pltpu.get_barrier_semaphore()
    for step in range(1, ranks):
        pl.semaphore_signal(
            barrier,
            inc=1,
            device_id={"orb": (me + step) % ranks},
            device_id_type=pl.DeviceIdType.MESH,
        )
    for step in range(1, REACH + 1):
        for shift in (step, groups - step):
            pl.semaphore_signal(
                barrier,
                inc=1,
                device_id={"pair": (group + shift) % groups},
                device_id_type=pl.DeviceIdType.MESH,
            )

    small_copies = [
        pltpu.make_async_copy(source_ref, target_ref, small_sem.at[at])
        for at, (source_ref, target_ref) in enumerate(
            (
                (amps_hbm, amplitudes),
                (first_hbm, occ_first),
                (second_hbm, occ_second),
                (energy_hbm, occ_energy),
                (pno_hbm, pno_energy),
                (couple_hbm, couple),
            )
        )
    ]
    small_copies[0].start()
    pl.semaphore_wait(barrier, ranks - 1 + 2 * REACH)

    def win_copy(turn, place, bare=False):
        return pltpu.make_async_remote_copy(
            src_ref=orb_hbm if bare else window.at[turn, middle],
            dst_ref=window.at[turn, pl.ds(place * orbs, orbs)],
            send_sem=win_send.at[turn],
            recv_sem=win_recv.at[turn, place],
            device_id={"pair": (group + REACH - place + groups) % groups},
            device_id_type=pl.DeviceIdType.MESH,
        )

    def amp_copy(turn, step, i):
        return pltpu.make_async_remote_copy(
            src_ref=amps.at[turn, own + i],
            dst_ref=amps.at[turn, own + i],
            send_sem=amp_send.at[turn],
            recv_sem=amp_recv.at[turn, step, i],
            device_id={"orb": target(step)},
            device_id_type=pl.DeviceIdType.MESH,
        )

    def amp_relay(turn, i):
        via, onto = (1, 2) if i % 2 == 0 else (2, 1)
        place = target(via) * own_pairs + i
        return pltpu.make_async_remote_copy(
            src_ref=amps.at[turn, place],
            dst_ref=amps.at[turn, place],
            send_sem=amp_send.at[turn],
            recv_sem=amp_recv.at[turn, 3, i],
            device_id={"orb": target(onto)},
            device_id_type=pl.DeviceIdType.MESH,
        )

    def relay_all(turn):
        for i in range(own_pairs):
            amp_copy(turn, 1 if i % 2 == 0 else 2, i).wait_recv()
            either(kinds(GATHER_DIRECT, turn), nothing, amp_relay(turn, i).start)

    def amp_wait(turn, step):
        for i in range(own_pairs):
            def wait(i=i):
                amp_copy(turn, step, i).wait_recv()

            if not square or step == 3 or (step, i % 2) in ((1, 1), (2, 0)):
                wait()

    def part_copy(turn, step, i):
        return pltpu.make_async_remote_copy(
            src_ref=parts_out.at[turn, i, step],
            dst_ref=parts_in.at[turn, i, step - 1],
            send_sem=part_send.at[turn],
            recv_sem=part_recv.at[turn, i],
            device_id={"orb": target(step)},
            device_id_type=pl.DeviceIdType.MESH,
        )

    def part_relay(turn, i):
        return pltpu.make_async_remote_copy(
            src_ref=parts_out.at[turn, i, 3],
            dst_ref=relayed.at[turn, i],
            send_sem=part_send.at[turn],
            recv_sem=relay_recv.at[turn, i],
            device_id={"orb": target(1 if i % 2 == 0 else 2)},
            device_id_type=pl.DeviceIdType.MESH,
        )

    def forward_all(turn):
        def relays():
            for i in range(own_pairs):
                onto = 2 if i % 2 == 0 else 1
                part_relay(turn, i).wait_recv()
                total = parts_out[turn, i, onto].astype(jnp.float32)
                total += relayed[turn, i].astype(jnp.float32)
                parts_out[turn, i, onto] = total.astype(bf16)
                part_copy(turn, onto, i).start()

        either(kinds(SUM_DIRECT, turn), nothing, relays)

    def whole(ref, send_sem, recv_sem):
        return pltpu.make_async_remote_copy(
            src_ref=ref,
            dst_ref=ref,
            send_sem=send_sem,
            recv_sem=recv_sem,
            device_id={"orb": target(1)},
            device_id_type=pl.DeviceIdType.MESH,
        )

    def part_wait(turn, i):
        def wait(terms):
            arrived = parts_in.at[turn, i, pl.ds(0, terms)]
            whole(arrived, part_send.at[turn], part_recv.at[turn, i]).wait_recv()

        if square:
            either(kinds(SUM_DIRECT, turn), lambda: wait(3), lambda: wait(2))
        else:
            wait(ranks - 1)

    def sent(turn):
        sends = pl.ds(0, (ranks - 1) * own_pairs)
        whole(amps.at[turn, sends], amp_send.at[turn], amp_recv.at[turn, 0, 0]).wait_send()
        sends = pl.ds(0, len(places) * orbs)
        whole(window.at[turn, sends], win_send.at[turn], win_recv.at[turn, 0]).wait_send()

    def parts_sent(turn):
        whole(parts_in.at[turn], part_send.at[turn], part_recv.at[turn, 0]).wait_send()

    def amp_start(turn, i):
        if square:
            either(kinds(GATHER_DIRECT, turn), amp_copy(turn, 3, i).start, nothing)
        for step in (1, 2) if square else range(ranks - 1, 0, -1):
            amp_copy(turn, step, i).start()

    def win_start(turn, bare=False):
        win_copy(turn, z_place, bare).start()
        win_copy(turn, c_place, bare).start()

    def transposed(turn):
        for o in range(orbs):
            blocks_t[o] = window[turn, REACH * orbs + o].T

    def integral(turn, step, i):
        pair = target(step) * own_pairs + i
        left = blocks_t[occ_first[pair] % orbs]
        parts_out[turn, i, step] = dot(left, blocks[second_at[pair]]).astype(bf16)

    def integrals(turn):
        for place in places:
            win_copy(turn, place).wait_recv()
        for at in range(SIDES * orbs):
            blocks[at] = window[turn, at]

        def one(i):
            for step in range(ranks - 1, -1, -1):
                integral(turn, step, i)
                if step > 0 and not square:
                    part_copy(turn, step, i).start()

        if square:
            for i in range(own_pairs):
                integral(turn, 3, i)
            for i in range(own_pairs):
                for step in (2, 1, 0):
                    integral(turn, step, i)
        else:
            pl.loop(0, own_pairs)(one)

    def far_sums(turn):
        def direct():
            for i in range(own_pairs):
                for step in (3, 1, 2):
                    part_copy(turn, step, i).start()

        def relays():
            for i in range(own_pairs):
                part_relay(turn, i).start()

        either(kinds(SUM_DIRECT, turn), direct, relays)

    def near_sums(turn):
        def relays():
            for i in range(own_pairs):
                part_copy(turn, 1 if i % 2 == 0 else 2, i).start()

        either(kinds(SUM_DIRECT, turn), nothing, relays)

    def through(turn, step):
        base = source(step) * own_pairs
        halves = []
        for i in range(own_pairs):
            amp = amps[turn, base + i]
            amps_now[base + i] = amp
            halves.append(dot(maps[base + i, 1], amp).astype(bf16))
        wholes = [dot(halves[i], first_t[base + i]) for i in range(own_pairs)]
        for i in range(own_pairs):
            local = occ_first[base + i] % orbs
            rows = pl.ds((step * own_pairs + i) * virtuals, virtuals)
            for o in range(orbs):
                masked = jnp.where(local == o, wholes[i], 0.0).astype(bf16)
                weights[rows, o * virtuals : (o + 1) * virtuals] = masked

    def applied(turn, some):
        lefts = [
            blocks[second_at[source(step) * own_pairs + i]]
            for step in some
            for i in range(own_pairs)
        ]
        rows = own_pairs * virtuals
        right = weights[pl.ds(some[0] * rows, len(some) * rows), :]
        return dot(jnp.concatenate(lefts, axis=1), right)

    def fit_near(turn):
        fitted[...] = applied(turn, near_steps)

    def dress(turn):
        if square:
            total = fitted[...] + applied(turn, far_steps)
        else:

            @pl.loop(1, ranks)
            def _(step):
                fitted[...] += applied(turn, (step,))

            total = fitted[...]
        values = [
            window[0, REACH * orbs + o].astype(jnp.float32)
            + dress_scale * total[:, o * virtuals : (o + 1) * virtuals]
            for o in range(orbs)
        ]

        @pl.when(turn + 1 < ITERS)
        def _():
            for o in range(orbs):
                window[turn + 1, REACH * orbs + o] = values[o].astype(bf16)

        @pl.when(turn + 1 == ITERS)
        def _():
            for o in range(orbs):
                out_dressed[o] = values[o]

    def couplings(turn):
        def one(i):
            halves = [
                dot(inter[i, k], amps_now[couple[i, k] % pairs]).astype(bf16)
                for k in range(partners)
            ]
            coupled[i] = dot(jnp.concatenate(halves, axis=1), inter_t[i])

        for i in range(own_pairs):
            one(i)

    def finish(turn):
        for first in range(0, own_pairs, BATCH):
            batch = range(first, min(first + BATCH, own_pairs))
            for i in batch:
                part_wait(turn, i)
            totals = {}
            for i in batch:
                total = parts_out[turn, i, 0].astype(jnp.float32)
                for step in range(1, ranks if SUM_DIRECT != NONE or not square else 3):
                    total += parts_in[turn, i, step - 1].astype(jnp.float32)
                totals[i] = total.astype(bf16)
            rights = {i: dot(totals[i], maps[own + i, 1]).astype(bf16) for i in batch}
            values = {
                i: (dot(first_t[own + i], rights[i]) + coupled[i]) * scale[i] for i in batch
            }

            @pl.when(turn + 1 < ITERS)
            def _(batch=batch, values=values):
                for i in batch:
                    amps[turn + 1, own + i] = values[i].astype(bf16)
                    amp_start(turn + 1, i)

            @pl.when(turn + 1 == ITERS)
            def _(batch=batch, values=values):
                for i in batch:
                    out_amps[i] = values[i]

    win_start(0, True)
    orb_copy = pltpu.make_async_copy(orb_hbm, window.at[0, middle], orb_sem)
    orb_copy.start()
    small_copies[0].wait()
    for i in range(own_pairs):
        amps[0, own + i] = amplitudes[i].astype(bf16)
    for i in range(own_pairs):
        amp_start(0, i)
    for copy in small_copies[1:]:
        copy.start()
    maps_copy = pltpu.make_async_copy(maps_hbm, maps, maps_sem)
    maps_copy.start()
    inter_copy = pltpu.make_async_copy(inter_hbm, inter, inter_sem)
    inter_copy.start()

    for copy in small_copies[1:]:
        copy.wait()

    @pl.loop(0, pairs)
    def _(pair):
        second = occ_second[pair]
        distance = (second // orbs - group + REACH + groups) % groups
        second_at[pair] = jnp.minimum(distance, SIDES - 1) * orbs + second % orbs

    if square and SUM_DIRECT != NONE:
        for turn in range(ITERS):

            def zero(turn=turn):
                for i in range(own_pairs):
                    parts_in[turn, i, 2] = jnp.zeros_like(parts_in[turn, i, 2])

            either(kinds(SUM_DIRECT, turn), nothing, zero)

    orb_copy.wait()
    transposed(0)
    maps_copy.wait()

    @pl.loop(0, ranks)
    def _(block):
        for i in range(own_pairs):
            first_t[block * own_pairs + i] = maps[block * own_pairs + i, 0].T

    inter_copy.wait()

    @pl.loop(0, own_pairs)
    def _(i):
        rows = jnp.broadcast_to(pno_energy[pl.ds(i, 1), :], (size, size))
        denominator = rows + rows.T
        denominator -= occ_energy[occ_first[own + i]]
        denominator -= occ_energy[occ_second[own + i]]
        scale[i] = -1.0 / denominator
        for k in range(partners):
            inter_t[i, k * size : (k + 1) * size, :] = inter[i, k].T

    near_steps = (0, 1, 2) if square else (0,)
    far_steps = (3,) if square else tuple(range(1, ranks))

    def throughs(turn, some):
        if square:
            for step in some:
                if step > 0:
                    amp_wait(turn, step)
        first, last = some[0], some[-1] + 1

        @pl.loop(first, last)
        def _(step):
            if not square and first > 0:
                amp_wait(turn, step)
            through(turn, step)

    near_steps = (0, 1, 2) if square else (0,)
    far_steps = (3,) if square else tuple(range(1, ranks))
    throughs(0, (0,))
    relay_first = {"all": True, "inner": inner, "none": False}[FIRST_RELAY]
    if square:
        either(relay_first, lambda: relay_all(0), nothing)

    def sums(turn, place):
        def some(far_place, near_place):
            if far_place == place:
                far_sums(turn)
            if near_place == place:
                near_sums(turn)

        either(inner, lambda: some(INNER_FAR, INNER_NEAR), lambda: some(0, 1))

    @pl.loop(0, ITERS)
    def _(turn):
        integrals(turn)

        if square:

            @pl.when(turn == 0)
            def _():
                far_sums(turn)
                either(relay_first, nothing, lambda: relay_all(0))

            @pl.when(turn > 0)
            def _():
                sums(turn, 0)
                throughs(turn, (0,))
                relay_all(turn)
                sums(turn, 1)

            throughs(turn, (1, 2))
        else:

            @pl.when(turn > 0)
            def _():
                throughs(turn, (0,))

        fit_near(turn)
        if square:

            @pl.when(turn > 0)
            def _():
                sums(turn, 2)
                forward_all(turn)

        throughs(turn, far_steps)
        dress(turn)

        @pl.when(turn + 1 < ITERS)
        def _():
            win_start(turn + 1)
            if square:
                near_sums(turn)
                forward_all(turn)
            transposed(turn + 1)

        couplings(turn)

        @pl.when(turn > 0)
        def _():
            sent(turn - 1)
            parts_sent(turn - 1)

        finish(turn)

    sent(ITERS - 1)
    parts_sent(ITERS - 1)


def store(amps, dressed, out_amps, out_dressed, sem):
    copies = [
        pltpu.make_async_copy(amps, out_amps, sem.at[0]),
        pltpu.make_async_copy(dressed, out_dressed, sem.at[1]),
    ]
    for copy in copies:
        copy.start()
    for copy in copies:
        copy.wait()


def on_device(
    ranks,
    groups,
    amplitudes,
    couple,
    occ_first,
    occ_second,
    couple_intersection,
    pno_maps,
    orbital_blocks,
    pno_energy,
    occ_energy,
):
    own_pairs, size, _ = amplitudes.shape
    group_pairs = occ_first.shape[0]
    orbs, rows, virtuals = orbital_blocks.shape
    partners = couple.shape[1]
    bf16 = jnp.bfloat16
    vmem = pl.BlockSpec(memory_space=pltpu.VMEM)
    hbm = pl.BlockSpec(memory_space=pltpu.HBM)
    dma = pltpu.SemaphoreType.DMA
    results = pl.pallas_call(
        functools.partial(kernel, ranks, groups),
        out_shape=(
            pltpu.VMEM(amplitudes.shape, jnp.float32),
            pltpu.VMEM(orbital_blocks.shape, jnp.float32),
        ),
        in_specs=[hbm] * 9,
        out_specs=(vmem, vmem),
        scratch_shapes=[
            pltpu.SMEM(couple.shape, couple.dtype),
            pltpu.SMEM(occ_first.shape, occ_first.dtype),
            pltpu.SMEM(occ_second.shape, occ_second.dtype),
            pltpu.SMEM(occ_energy.shape, occ_energy.dtype),
            pltpu.SMEM(occ_second.shape, occ_second.dtype),
            pltpu.VMEM(amplitudes.shape, amplitudes.dtype),
            pltpu.VMEM(pno_energy.shape, pno_energy.dtype),
            pltpu.VMEM(couple_intersection.shape, bf16),
            pltpu.VMEM((own_pairs, partners * size, size), bf16),
            pltpu.VMEM(pno_maps.shape, bf16),
            pltpu.VMEM((group_pairs, size, virtuals), bf16),
            pltpu.VMEM((orbs, virtuals, rows), bf16),
            pltpu.VMEM((own_pairs, size, size), jnp.float32),
            pltpu.VMEM((own_pairs, size, size), jnp.float32),
            pltpu.VMEM((ITERS, group_pairs, size, size), bf16),
            pltpu.VMEM((group_pairs, size, size), bf16),
            pltpu.VMEM((ITERS, SIDES * orbs, rows, virtuals), bf16),
            pltpu.VMEM((SIDES * orbs, rows, virtuals), bf16),
            pltpu.VMEM((ITERS, own_pairs, ranks, virtuals, virtuals), bf16),
            pltpu.VMEM((ITERS, own_pairs, ranks - 1, virtuals, virtuals), bf16),
            pltpu.VMEM((ITERS, own_pairs, virtuals, virtuals), bf16),
            pltpu.VMEM((group_pairs * virtuals, orbs * virtuals), bf16),
            pltpu.VMEM((rows, orbs * virtuals), jnp.float32),
            dma((ITERS,)),
            dma((ITERS, ranks, own_pairs)),
            dma((ITERS,)),
            dma((ITERS, SIDES)),
            dma((ITERS,)),
            dma((ITERS, own_pairs)),
            dma((ITERS, own_pairs)),
            dma,
            dma,
            dma,
            dma((6,)),
        ],
        compiler_params=pltpu.CompilerParams(
            collective_id=0, has_side_effects=True, vmem_limit_bytes=67043328 - 4096 * 1024
        ),
    )(
        *(pltpu.with_memory_space_constraint(x, pltpu.HBM) for x in (
        couple,
        occ_first,
        occ_second,
        occ_energy,
        amplitudes,
        pno_energy,
        couple_intersection,
        pno_maps,
        orbital_blocks,
        ))
    )
    return pl.pallas_call(
        store,
        out_shape=tuple(pltpu.HBM(x.shape, x.dtype) for x in results),
        in_specs=[vmem] * 2,
        out_specs=(hbm, hbm),
        scratch_shapes=[dma((2,))],
        compiler_params=pltpu.CompilerParams(vmem_limit_bytes=4096 * 1024),
    )(*(pltpu.with_memory_space_constraint(x, pltpu.VMEM) for x in results))


def solution(mesh):
    return jax.shard_map(
        functools.partial(on_device, mesh.shape["orb"], mesh.shape["pair"]),
        mesh=mesh,
        in_specs=(
            P(("pair", "orb"), None, None),
            P(("pair", "orb"), None),
            P("pair"),
            P("pair"),
            P(("pair", "orb"), None, None, None),
            P("pair", None, None, None),
            P("pair", "orb", None),
            P(("pair", "orb"), None),
            P(),
        ),
        out_specs=(P(("pair", "orb"), None, None), P("pair", "orb", None)),
        check_vma=False,
    )
```

```python
import functools

import jax
import jax.numpy as jnp
from jax import lax
from jax.experimental import pallas as pl
from jax.experimental.pallas import tpu as pltpu
from jax.sharding import PartitionSpec as P

REACH = 1
ITERS = 2
SIDES = 2 * REACH + 1

dress_scale = 0.015
BATCH = 2
SUM_DIRECT = ("outer", "none")
NONE = ("none", "none")
FIRST_RELAY = "all"
EARLY_NEAR = True
NEAR_AT = 0
INNER_FAR = 1
INNER_NEAR = 2

NN = (((1,), (0,)), ((), ()))
NT = (((1,), (1,)), ((), ()))


def dot(left, right, dims=NN):
    return lax.dot_general(left, right, dims, preferred_element_type=jnp.float32)


def kernel(
    ranks,
    groups,
    couple_hbm,
    first_hbm,
    second_hbm,
    energy_hbm,
    amps_hbm,
    pno_hbm,
    inter_hbm,
    maps_hbm,
    orb_hbm,
    out_amps,
    out_dressed,
    couple,
    occ_first,
    occ_second,
    occ_energy,
    second_at,
    amplitudes,
    pno_energy,
    inter,
    inter_t,
    maps,
    first_t,
    blocks_t,
    scale,
    coupled,
    amps,
    amps_now,
    window,
    blocks,
    parts_out,
    parts_in,
    relayed,
    weights,
    fitted,
    amp_send,
    amp_recv,
    win_send,
    win_recv,
    part_send,
    part_recv,
    relay_recv,
    inter_sem,
    maps_sem,
    orb_sem,
    small_sem,
):
    own_pairs = amps_hbm.shape[0]
    orbs = orb_hbm.shape[0]
    partners = couple.shape[1]
    size = amplitudes.shape[2]
    virtuals = orb_hbm.shape[2]
    pairs = ranks * own_pairs
    me = lax.axis_index("orb")
    group = lax.axis_index("pair")
    own = me * own_pairs
    middle = pl.ds(REACH * orbs, orbs)
    places = [place for place in range(SIDES) if place != REACH]
    bf16 = jnp.bfloat16
    square = ranks == 4 and own_pairs % BATCH == 0
    z_place = (group + 1) % 2 * 2 * REACH
    c_place = 2 * REACH - z_place

    def target(step):
        if square:
            return (me // 2 + step // 2) % 2 * 2 + (me + step) % 2
        return (me + step) % ranks

    def source(step):
        return target(step) if square else (me + ranks - step) % ranks

    inner = group % 2 == 1

    def kinds(modes, turn):
        flags = [{"none": False, "all": True, "outer": jnp.logical_not(inner)}[m] for m in modes]
        if isinstance(turn, int):
            return flags[turn]
        if all(mode == modes[0] for mode in modes):
            return flags[0]
        flag = False
        for at in range(ITERS):
            flag = jnp.logical_or(flag, jnp.logical_and(turn == at, flags[at]))
        return flag

    def either(flag, yes, no):
        if isinstance(flag, bool):
            (yes if flag else no)()
        else:
            pl.when(flag)(yes)
            pl.when(jnp.logical_not(flag))(no)

    def nothing():
        pass

    barrier = pltpu.get_barrier_semaphore()
    for step in range(1, ranks):
        pl.semaphore_signal(
            barrier,
            inc=1,
            device_id={"orb": (me + step) % ranks},
            device_id_type=pl.DeviceIdType.MESH,
        )
    for step in range(1, REACH + 1):
        for shift in (step, groups - step):
            pl.semaphore_signal(
                barrier,
                inc=1,
                device_id={"pair": (group + shift) % groups},
                device_id_type=pl.DeviceIdType.MESH,
            )

    small_copies = [
        pltpu.make_async_copy(source_ref, target_ref, small_sem.at[at])
        for at, (source_ref, target_ref) in enumerate(
            (
                (amps_hbm, amplitudes),
                (first_hbm, occ_first),
                (second_hbm, occ_second),
                (energy_hbm, occ_energy),
                (pno_hbm, pno_energy),
                (couple_hbm, couple),
            )
        )
    ]
    small_copies[0].start()
    pl.semaphore_wait(barrier, ranks - 1 + 2 * REACH)

    def win_copy(turn, place, bare=False):
        return pltpu.make_async_remote_copy(
            src_ref=orb_hbm if bare else window.at[turn, middle],
            dst_ref=window.at[turn, pl.ds(place * orbs, orbs)],
            send_sem=win_send.at[turn],
            recv_sem=win_recv.at[turn],
            device_id={"pair": (group + REACH - place + groups) % groups},
            device_id_type=pl.DeviceIdType.MESH,
        )

    def relayed_tile(step, i):
        return (step, i % 2) in ((1, 0), (2, 1))

    def amp_slot(step, i):
        if not square:
            return step
        return i if relayed_tile(step, i) else own_pairs

    def amp_copy(turn, step, i):
        return pltpu.make_async_remote_copy(
            src_ref=amps.at[turn, own + i],
            dst_ref=amps.at[turn, own + i],
            send_sem=amp_send.at[turn],
            recv_sem=amp_recv.at[turn, amp_slot(step, i)],
            device_id={"orb": target(step)},
            device_id_type=pl.DeviceIdType.MESH,
        )

    def amp_relay(turn, i):
        via, onto = (1, 2) if i % 2 == 0 else (2, 1)
        place = target(via) * own_pairs + i
        return pltpu.make_async_remote_copy(
            src_ref=amps.at[turn, place],
            dst_ref=amps.at[turn, place],
            send_sem=amp_send.at[turn],
            recv_sem=amp_recv.at[turn, own_pairs + 1],
            device_id={"orb": target(onto)},
            device_id_type=pl.DeviceIdType.MESH,
        )

    def relay_all(turn):
        for i in range(own_pairs):
            amp_copy(turn, 1 if i % 2 == 0 else 2, i).wait_recv()
            amp_relay(turn, i).start()

    def amp_wait(turn, slot):
        block = amps.at[turn, pl.ds(own, own_pairs)]
        whole(block, amp_send.at[turn], amp_recv.at[turn, slot]).wait_recv()

    def part_copy(turn, step, i):
        return pltpu.make_async_remote_copy(
            src_ref=parts_out.at[turn, i, step],
            dst_ref=parts_in.at[turn, i // BATCH, step - 1, i % BATCH],
            send_sem=part_send.at[turn],
            recv_sem=part_recv.at[turn, i // BATCH],
            device_id={"orb": target(step)},
            device_id_type=pl.DeviceIdType.MESH,
        )

    def part_relay(turn, i):
        return pltpu.make_async_remote_copy(
            src_ref=parts_out.at[turn, i, 3],
            dst_ref=relayed.at[turn, i],
            send_sem=part_send.at[turn],
            recv_sem=relay_recv.at[turn, i // BATCH],
            device_id={"orb": target(1 if i % 2 == 0 else 2)},
            device_id_type=pl.DeviceIdType.MESH,
        )

    def forward_all(turn):
        def relays():
            for first in range(0, own_pairs, BATCH):
                arrived = relayed.at[turn, pl.ds(first, BATCH)]
                whole(arrived, part_send.at[turn], relay_recv.at[turn, first // BATCH]).wait_recv()
                for i in range(first, first + BATCH):
                    onto = 2 if i % 2 == 0 else 1
                    total = parts_out[turn, i, onto].astype(jnp.float32)
                    total += relayed[turn, i].astype(jnp.float32)
                    parts_out[turn, i, onto] = total.astype(bf16)
                for i in range(first, first + BATCH):
                    part_copy(turn, 2 if i % 2 == 0 else 1, i).start()

        either(kinds(SUM_DIRECT, turn), nothing, relays)

    def whole(ref, send_sem, recv_sem):
        return pltpu.make_async_remote_copy(
            src_ref=ref,
            dst_ref=ref,
            send_sem=send_sem,
            recv_sem=recv_sem,
            device_id={"orb": target(1)},
            device_id_type=pl.DeviceIdType.MESH,
        )

    def part_wait(turn, at):
        def wait(terms):
            arrived = parts_in.at[turn, at, pl.ds(0, terms)]
            whole(arrived, part_send.at[turn], part_recv.at[turn, at]).wait_recv()

        if square:
            either(kinds(SUM_DIRECT, turn), lambda: wait(3), lambda: wait(2))
        else:
            wait(ranks - 1)

    def sent(turn):
        sends = pl.ds(0, (ranks - 1) * own_pairs)
        whole(amps.at[turn, sends], amp_send.at[turn], amp_recv.at[turn, 0]).wait_send()
        sends = pl.ds(0, len(places) * orbs)
        whole(window.at[turn, sends], win_send.at[turn], win_recv.at[turn]).wait_send()

    def parts_sent(turn):
        whole(parts_in.at[turn], part_send.at[turn], part_recv.at[turn, 0]).wait_send()

    def amp_start(turn, i):
        for step in range(ranks - 1, 0, -1):
            amp_copy(turn, step, i).start()

    def amps_start(turn, batch):
        if square:
            for turned in (0, 1):
                for i in batch:
                    amp_copy(turn, 1 if (i + turned) % 2 == 0 else 2, i).start()
        else:
            for i in batch:
                amp_start(turn, i)

    def win_start(turn, bare=False):
        win_copy(turn, z_place, bare).start()
        win_copy(turn, c_place, bare).start()

    def transposed(turn):
        for o in range(orbs):
            blocks_t[o] = window[turn, REACH * orbs + o].T

    def integral(turn, step, i):
        pair = target(step) * own_pairs + i
        left = blocks_t[occ_first[pair] % orbs]
        parts_out[turn, i, step] = dot(left, blocks[second_at[pair]]).astype(bf16)

    def integrals(turn):
        arrivals = window.at[turn, pl.ds(0, len(places) * orbs)]
        whole(arrivals, win_send.at[turn], win_recv.at[turn]).wait_recv()
        for at in range(SIDES * orbs):
            blocks[at] = window[turn, at]

        def one(i):
            for step in range(ranks - 1, -1, -1):
                integral(turn, step, i)
                if step > 0 and not square:
                    part_copy(turn, step, i).start()

        if square:
            for i in range(own_pairs):
                integral(turn, 3, i)
            for i in range(own_pairs):
                for step in (2, 1, 0):
                    integral(turn, step, i)
        else:
            pl.loop(0, own_pairs)(one)

    def far_sums(turn):
        def direct():
            for i in range(own_pairs):
                for step in (3, 1, 2):
                    part_copy(turn, step, i).start()

        def relays():
            for i in range(own_pairs):
                part_relay(turn, i).start()

        either(kinds(SUM_DIRECT, turn), direct, relays)

    def near_sums(turn):
        def relays():
            for i in range(own_pairs):
                part_copy(turn, 1 if i % 2 == 0 else 2, i).start()

        either(kinds(SUM_DIRECT, turn), nothing, relays)

    def through(turn, step):
        base = source(step) * own_pairs
        halves = []
        for i in range(own_pairs):
            amp = amps[turn, base + i]
            amps_now[base + i] = amp
            halves.append(dot(maps[base + i, 1], amp).astype(bf16))
        wholes = [dot(halves[i], first_t[base + i]) for i in range(own_pairs)]
        for i in range(own_pairs):
            local = occ_first[base + i] % orbs
            rows = pl.ds((step * own_pairs + i) * virtuals, virtuals)
            for o in range(orbs):
                masked = jnp.where(local == o, wholes[i], 0.0).astype(bf16)
                weights[rows, o * virtuals : (o + 1) * virtuals] = masked

    def applied(turn, some):
        lefts = [
            blocks[second_at[source(step) * own_pairs + i]]
            for step in some
            for i in range(own_pairs)
        ]
        rows = own_pairs * virtuals
        right = weights[pl.ds(some[0] * rows, len(some) * rows), :]
        return dot(jnp.concatenate(lefts, axis=1), right)

    def fit_near(turn):
        fitted[...] = applied(turn, near_steps)

    def dress(turn):
        if square:
            total = fitted[...] + applied(turn, far_steps)
        else:

            @pl.loop(1, ranks)
            def _(step):
                fitted[...] += applied(turn, (step,))

            total = fitted[...]
        values = [
            window[0, REACH * orbs + o].astype(jnp.float32)
            + dress_scale * total[:, o * virtuals : (o + 1) * virtuals]
            for o in range(orbs)
        ]

        @pl.when(turn + 1 < ITERS)
        def _():
            for o in range(orbs):
                window[turn + 1, REACH * orbs + o] = values[o].astype(bf16)

        @pl.when(turn + 1 == ITERS)
        def _():
            for o in range(orbs):
                out_dressed[o] = values[o]

    def couplings(turn):
        def one(i):
            halves = [
                dot(inter[i, k], amps_now[couple[i, k] % pairs]).astype(bf16)
                for k in range(partners)
            ]
            coupled[i] = dot(jnp.concatenate(halves, axis=1), inter_t[i])

        for i in range(own_pairs):
            one(i)

    def finish(turn):
        for first in range(0, own_pairs, BATCH):
            batch = range(first, min(first + BATCH, own_pairs))
            part_wait(turn, first // BATCH)
            totals = {}
            for i in batch:
                total = parts_out[turn, i, 0].astype(jnp.float32)
                for step in range(1, ranks if SUM_DIRECT != NONE or not square else 3):
                    total += parts_in[turn, i // BATCH, step - 1, i % BATCH].astype(jnp.float32)
                totals[i] = total.astype(bf16)
            rights = {i: dot(totals[i], maps[own + i, 1]).astype(bf16) for i in batch}
            values = {
                i: (dot(first_t[own + i], rights[i]) + coupled[i]) * scale[i] for i in batch
            }

            @pl.when(turn + 1 < ITERS)
            def _(batch=batch, values=values):
                for i in batch:
                    amps[turn + 1, own + i] = values[i].astype(bf16)
                amps_start(turn + 1, batch)

            @pl.when(turn + 1 == ITERS)
            def _(batch=batch, values=values):
                for i in batch:
                    out_amps[i] = values[i]

    win_start(0, True)
    orb_copy = pltpu.make_async_copy(orb_hbm, window.at[0, middle], orb_sem)
    orb_copy.start()
    small_copies[0].wait()
    for i in range(own_pairs):
        amps[0, own + i] = amplitudes[i].astype(bf16)
    amps_start(0, range(own_pairs))
    for copy in small_copies[1:]:
        copy.start()
    maps_copy = pltpu.make_async_copy(maps_hbm, maps, maps_sem)
    maps_copy.start()
    inter_copy = pltpu.make_async_copy(inter_hbm, inter, inter_sem)
    inter_copy.start()

    for copy in small_copies[1:]:
        copy.wait()

    @pl.loop(0, pairs)
    def _(pair):
        second = occ_second[pair]
        distance = (second // orbs - group + REACH + groups) % groups
        second_at[pair] = jnp.minimum(distance, SIDES - 1) * orbs + second % orbs

    if square and SUM_DIRECT != NONE:
        for turn in range(ITERS):

            def zero(turn=turn):
                for i in range(own_pairs):
                    parts_in[turn, i // BATCH, 2, i % BATCH] = jnp.zeros((size, size), bf16)

            either(kinds(SUM_DIRECT, turn), nothing, zero)

    orb_copy.wait()
    transposed(0)
    maps_copy.wait()

    @pl.loop(0, ranks)
    def _(block):
        for i in range(own_pairs):
            first_t[block * own_pairs + i] = maps[block * own_pairs + i, 0].T

    inter_copy.wait()

    @pl.loop(0, own_pairs)
    def _(i):
        rows = jnp.broadcast_to(pno_energy[pl.ds(i, 1), :], (size, size))
        denominator = rows + rows.T
        denominator -= occ_energy[occ_first[own + i]]
        denominator -= occ_energy[occ_second[own + i]]
        scale[i] = -1.0 / denominator
        for k in range(partners):
            inter_t[i, k * size : (k + 1) * size, :] = inter[i, k].T

    near_steps = (0, 1, 2) if square else (0,)
    far_steps = (3,) if square else tuple(range(1, ranks))

    def throughs(turn, some):
        first, last = some[0], some[-1] + 1
        if square and first > 0:
            amp_wait(turn, own_pairs + (0 if first == 1 else 1))

        @pl.loop(first, last)
        def _(step):
            if not square and first > 0:
                amp_wait(turn, step)
            through(turn, step)

    near_steps = (0, 1, 2) if square else (0,)
    far_steps = (3,) if square else tuple(range(1, ranks))
    throughs(0, (0,))
    relay_first = {"all": True, "inner": inner, "none": False}[FIRST_RELAY]
    if square:
        either(relay_first, lambda: relay_all(0), nothing)
        if EARLY_NEAR:
            either(inner, lambda: throughs(0, (1, 2)), nothing)

    def sums(turn, place):
        def some(far_place, near_place):
            if far_place == place:
                far_sums(turn)
            if near_place == place:
                near_sums(turn)

        either(inner, lambda: some(INNER_FAR, INNER_NEAR), lambda: some(0, 1))

    @pl.loop(0, ITERS)
    def _(turn):
        integrals(turn)

        if square:

            @pl.when(turn == 0)
            def _():
                far_sums(turn)
                if NEAR_AT == 0:
                    near_sums(turn)

            @pl.when(turn > 0)
            def _():
                sums(turn, 0)
                throughs(turn, (0,))
                relay_all(turn)
                sums(turn, 1)

            if EARLY_NEAR:

                @pl.when(jnp.logical_or(turn > 0, jnp.logical_not(inner)))
                def _():
                    throughs(turn, (1, 2))

            else:
                throughs(turn, (1, 2))
        else:

            @pl.when(turn > 0)
            def _():
                throughs(turn, (0,))

        fit_near(turn)
        if square:

            @pl.when(turn > 0)
            def _():
                sums(turn, 2)
                forward_all(turn)

        throughs(turn, far_steps)
        dress(turn)

        @pl.when(turn + 1 < ITERS)
        def _():
            win_start(turn + 1)
            if square:
                if NEAR_AT == 1:
                    near_sums(turn)
                forward_all(turn)
                if NEAR_AT == 2:
                    near_sums(turn)
            transposed(turn + 1)

        couplings(turn)

        @pl.when(turn > 0)
        def _():
            sent(turn - 1)
            parts_sent(turn - 1)

        finish(turn)

    sent(ITERS - 1)
    parts_sent(ITERS - 1)


def store(amps, dressed, out_amps, out_dressed, sem):
    copies = [
        pltpu.make_async_copy(amps, out_amps, sem.at[0]),
        pltpu.make_async_copy(dressed, out_dressed, sem.at[1]),
    ]
    for copy in copies:
        copy.start()
    for copy in copies:
        copy.wait()


def on_device(
    ranks,
    groups,
    amplitudes,
    couple,
    occ_first,
    occ_second,
    couple_intersection,
    pno_maps,
    orbital_blocks,
    pno_energy,
    occ_energy,
):
    own_pairs, size, _ = amplitudes.shape
    group_pairs = occ_first.shape[0]
    orbs, rows, virtuals = orbital_blocks.shape
    partners = couple.shape[1]
    bf16 = jnp.bfloat16
    vmem = pl.BlockSpec(memory_space=pltpu.VMEM)
    hbm = pl.BlockSpec(memory_space=pltpu.HBM)
    dma = pltpu.SemaphoreType.DMA
    square = ranks == 4 and own_pairs % BATCH == 0
    results = pl.pallas_call(
        functools.partial(kernel, ranks, groups),
        out_shape=(
            pltpu.VMEM(amplitudes.shape, jnp.float32),
            pltpu.VMEM(orbital_blocks.shape, jnp.float32),
        ),
        in_specs=[hbm] * 9,
        out_specs=(vmem, vmem),
        scratch_shapes=[
            pltpu.SMEM(couple.shape, couple.dtype),
            pltpu.SMEM(occ_first.shape, occ_first.dtype),
            pltpu.SMEM(occ_second.shape, occ_second.dtype),
            pltpu.SMEM(occ_energy.shape, occ_energy.dtype),
            pltpu.SMEM(occ_second.shape, occ_second.dtype),
            pltpu.VMEM(amplitudes.shape, amplitudes.dtype),
            pltpu.VMEM(pno_energy.shape, pno_energy.dtype),
            pltpu.VMEM(couple_intersection.shape, bf16),
            pltpu.VMEM((own_pairs, partners * size, size), bf16),
            pltpu.VMEM(pno_maps.shape, bf16),
            pltpu.VMEM((group_pairs, size, virtuals), bf16),
            pltpu.VMEM((orbs, virtuals, rows), bf16),
            pltpu.VMEM((own_pairs, size, size), jnp.float32),
            pltpu.VMEM((own_pairs, size, size), jnp.float32),
            pltpu.VMEM((ITERS, group_pairs, size, size), bf16),
            pltpu.VMEM((group_pairs, size, size), bf16),
            pltpu.VMEM((ITERS, SIDES * orbs, rows, virtuals), bf16),
            pltpu.VMEM((SIDES * orbs, rows, virtuals), bf16),
            pltpu.VMEM((ITERS, own_pairs, ranks, virtuals, virtuals), bf16),
            pltpu.VMEM((ITERS, own_pairs // BATCH, ranks - 1, BATCH, virtuals, virtuals), bf16),
            pltpu.VMEM((ITERS, own_pairs, virtuals, virtuals), bf16),
            pltpu.VMEM((group_pairs * virtuals, orbs * virtuals), bf16),
            pltpu.VMEM((rows, orbs * virtuals), jnp.float32),
            dma((ITERS,)),
            dma((ITERS, own_pairs + 2 if square else ranks)),
            dma((ITERS,)),
            dma((ITERS,)),
            dma((ITERS,)),
            dma((ITERS, own_pairs // BATCH)),
            dma((ITERS, own_pairs // BATCH)),
            dma,
            dma,
            dma,
            dma((6,)),
        ],
        compiler_params=pltpu.CompilerParams(
            collective_id=0, has_side_effects=True, vmem_limit_bytes=67043328 - 4096 * 1024
        ),
    )(
        *(pltpu.with_memory_space_constraint(x, pltpu.HBM) for x in (
        couple,
        occ_first,
        occ_second,
        occ_energy,
        amplitudes,
        pno_energy,
        couple_intersection,
        pno_maps,
        orbital_blocks,
        ))
    )
    return pl.pallas_call(
        store,
        out_shape=tuple(pltpu.HBM(x.shape, x.dtype) for x in results),
        in_specs=[vmem] * 2,
        out_specs=(hbm, hbm),
        scratch_shapes=[dma((2,))],
        compiler_params=pltpu.CompilerParams(vmem_limit_bytes=4096 * 1024),
    )(*(pltpu.with_memory_space_constraint(x, pltpu.VMEM) for x in results))


def solution(mesh):
    return jax.shard_map(
        functools.partial(on_device, mesh.shape["orb"], mesh.shape["pair"]),
        mesh=mesh,
        in_specs=(
            P(("pair", "orb"), None, None),
            P(("pair", "orb"), None),
            P("pair"),
            P("pair"),
            P(("pair", "orb"), None, None, None),
            P("pair", None, None, None),
            P("pair", "orb", None),
            P(("pair", "orb"), None),
            P(),
        ),
        out_specs=(P(("pair", "orb"), None, None), P("pair", "orb", None)),
        check_vma=False,
    )
```

```python
import functools

import jax
import jax.numpy as jnp
from jax import lax
from jax.experimental import pallas as pl
from jax.experimental.pallas import tpu as pltpu
from jax.sharding import PartitionSpec as P

REACH = 1
ITERS = 2
SIDES = 2 * REACH + 1

dress_scale = 0.015
BATCH = 2
SUM_DIRECT = ("outer", "none")
NONE = ("none", "none")
FIRST_RELAY = "all"
EARLY_NEAR = True
NEAR_AT = 0
INNER_FAR = 1
INNER_NEAR = 2

NN = (((1,), (0,)), ((), ()))
NT = (((1,), (1,)), ((), ()))


def dot(left, right, dims=NN):
    return lax.dot_general(left, right, dims, preferred_element_type=jnp.float32)


def kernel(
    ranks,
    groups,
    couple_hbm,
    first_hbm,
    second_hbm,
    energy_hbm,
    amps_hbm,
    pno_hbm,
    inter_hbm,
    maps_hbm,
    orb_hbm,
    out_amps,
    out_dressed,
    couple,
    occ_first,
    occ_second,
    occ_energy,
    second_at,
    amplitudes,
    pno_energy,
    inter,
    inter_t,
    maps,
    first_t,
    blocks_t,
    scale,
    coupled,
    amps,
    amps_now,
    window,
    blocks,
    parts_out,
    parts_in,
    relayed,
    weights,
    fitted,
    amp_send,
    amp_recv,
    win_send,
    win_recv,
    part_send,
    part_recv,
    relay_recv,
    inter_sem,
    maps_sem,
    orb_sem,
    small_sem,
):
    own_pairs = amps_hbm.shape[0]
    orbs = orb_hbm.shape[0]
    partners = couple.shape[1]
    size = amplitudes.shape[2]
    virtuals = orb_hbm.shape[2]
    pairs = ranks * own_pairs
    me = lax.axis_index("orb")
    group = lax.axis_index("pair")
    own = me * own_pairs
    middle = pl.ds(REACH * orbs, orbs)
    places = [place for place in range(SIDES) if place != REACH]
    bf16 = jnp.bfloat16
    square = ranks == 4 and own_pairs % BATCH == 0
    z_place = (group + 1) % 2 * 2 * REACH
    c_place = 2 * REACH - z_place

    def target(step):
        if square:
            return (me // 2 + step // 2) % 2 * 2 + (me + step) % 2
        return (me + step) % ranks

    def source(step):
        return target(step) if square else (me + ranks - step) % ranks

    inner = group % 2 == 1

    def kinds(modes, turn):
        flags = [{"none": False, "all": True, "outer": jnp.logical_not(inner)}[m] for m in modes]
        if isinstance(turn, int):
            return flags[turn]
        if all(mode == modes[0] for mode in modes):
            return flags[0]
        flag = False
        for at in range(ITERS):
            flag = jnp.logical_or(flag, jnp.logical_and(turn == at, flags[at]))
        return flag

    def either(flag, yes, no):
        if isinstance(flag, bool):
            (yes if flag else no)()
        else:
            pl.when(flag)(yes)
            pl.when(jnp.logical_not(flag))(no)

    def nothing():
        pass

    barrier = pltpu.get_barrier_semaphore()
    for step in range(1, ranks):
        pl.semaphore_signal(
            barrier,
            inc=1,
            device_id={"orb": (me + step) % ranks},
            device_id_type=pl.DeviceIdType.MESH,
        )
    for step in range(1, REACH + 1):
        for shift in (step, groups - step):
            pl.semaphore_signal(
                barrier,
                inc=1,
                device_id={"pair": (group + shift) % groups},
                device_id_type=pl.DeviceIdType.MESH,
            )

    small_copies = [
        pltpu.make_async_copy(source_ref, target_ref, small_sem.at[at])
        for at, (source_ref, target_ref) in enumerate(
            (
                (amps_hbm, amplitudes),
                (first_hbm, occ_first),
                (second_hbm, occ_second),
                (energy_hbm, occ_energy),
                (pno_hbm, pno_energy),
                (couple_hbm, couple),
            )
        )
    ]
    small_copies[0].start()
    pl.semaphore_wait(barrier, ranks - 1 + 2 * REACH)

    def win_copy(turn, place, bare=False):
        return pltpu.make_async_remote_copy(
            src_ref=orb_hbm if bare else window.at[turn, middle],
            dst_ref=window.at[turn, pl.ds(place * orbs, orbs)],
            send_sem=win_send.at[turn],
            recv_sem=win_recv.at[turn],
            device_id={"pair": (group + REACH - place + groups) % groups},
            device_id_type=pl.DeviceIdType.MESH,
        )

    def relayed_tile(step, i):
        return (step, i % 2) in ((1, 0), (2, 1))

    def amp_slot(step, i):
        if not square:
            return step
        return i if relayed_tile(step, i) else own_pairs

    def amp_copy(turn, step, i):
        return pltpu.make_async_remote_copy(
            src_ref=amps.at[turn, own + i],
            dst_ref=amps.at[turn, own + i],
            send_sem=amp_send.at[turn],
            recv_sem=amp_recv.at[turn, amp_slot(step, i)],
            device_id={"orb": target(step)},
            device_id_type=pl.DeviceIdType.MESH,
        )

    def amp_relay(turn, i):
        via, onto = (1, 2) if i % 2 == 0 else (2, 1)
        place = target(via) * own_pairs + i
        return pltpu.make_async_remote_copy(
            src_ref=amps.at[turn, place],
            dst_ref=amps.at[turn, place],
            send_sem=amp_send.at[turn],
            recv_sem=amp_recv.at[turn, own_pairs + 1],
            device_id={"orb": target(onto)},
            device_id_type=pl.DeviceIdType.MESH,
        )

    def relay_all(turn):
        for i in range(own_pairs):
            amp_copy(turn, 1 if i % 2 == 0 else 2, i).wait_recv()
            amp_relay(turn, i).start()

    def amp_wait(turn, slot):
        block = amps.at[turn, pl.ds(own, own_pairs)]
        whole(block, amp_send.at[turn], amp_recv.at[turn, slot]).wait_recv()

    def part_copy(turn, step, i):
        return pltpu.make_async_remote_copy(
            src_ref=parts_out.at[turn, i, step],
            dst_ref=parts_in.at[turn, i // BATCH, step - 1, i % BATCH],
            send_sem=part_send.at[turn],
            recv_sem=part_recv.at[turn, i // BATCH],
            device_id={"orb": target(step)},
            device_id_type=pl.DeviceIdType.MESH,
        )

    def part_relay(turn, i):
        return pltpu.make_async_remote_copy(
            src_ref=parts_out.at[turn, i, 3],
            dst_ref=relayed.at[turn, i],
            send_sem=part_send.at[turn],
            recv_sem=relay_recv.at[turn, i // BATCH],
            device_id={"orb": target(1 if i % 2 == 0 else 2)},
            device_id_type=pl.DeviceIdType.MESH,
        )

    def forward_all(turn):
        def relays():
            for first in range(0, own_pairs, BATCH):
                arrived = relayed.at[turn, pl.ds(first, BATCH)]
                whole(arrived, part_send.at[turn], relay_recv.at[turn, first // BATCH]).wait_recv()
                for i in range(first, first + BATCH):
                    onto = 2 if i % 2 == 0 else 1
                    total = parts_out[turn, i, onto].astype(jnp.float32)
                    total += relayed[turn, i].astype(jnp.float32)
                    parts_out[turn, i, onto] = total.astype(bf16)
                for i in range(first, first + BATCH):
                    part_copy(turn, 2 if i % 2 == 0 else 1, i).start()

        either(kinds(SUM_DIRECT, turn), nothing, relays)

    def whole(ref, send_sem, recv_sem):
        return pltpu.make_async_remote_copy(
            src_ref=ref,
            dst_ref=ref,
            send_sem=send_sem,
            recv_sem=recv_sem,
            device_id={"orb": target(1)},
            device_id_type=pl.DeviceIdType.MESH,
        )

    def part_wait(turn, at):
        def wait(terms):
            arrived = parts_in.at[turn, at, pl.ds(0, terms)]
            whole(arrived, part_send.at[turn], part_recv.at[turn, at]).wait_recv()

        if square:
            either(kinds(SUM_DIRECT, turn), lambda: wait(3), lambda: wait(2))
        else:
            wait(ranks - 1)

    def sent(turn):
        sends = pl.ds(0, (ranks - 1) * own_pairs)
        whole(amps.at[turn, sends], amp_send.at[turn], amp_recv.at[turn, 0]).wait_send()
        sends = pl.ds(0, len(places) * orbs)
        whole(window.at[turn, sends], win_send.at[turn], win_recv.at[turn]).wait_send()

    def parts_sent(turn):
        whole(parts_in.at[turn], part_send.at[turn], part_recv.at[turn, 0]).wait_send()

    def amp_start(turn, i):
        for step in range(ranks - 1, 0, -1):
            amp_copy(turn, step, i).start()

    def amps_start(turn, batch):
        if square:
            for turned in (0, 1):
                for i in batch:
                    amp_copy(turn, 1 if (i + turned) % 2 == 0 else 2, i).start()
        else:
            for i in batch:
                amp_start(turn, i)

    def win_start(turn, bare=False):
        win_copy(turn, c_place, bare).start()
        win_copy(turn, z_place, bare).start()

    def transposed(turn):
        for o in range(orbs):
            blocks_t[o] = window[turn, REACH * orbs + o].T

    def integral(turn, step, i):
        pair = target(step) * own_pairs + i
        left = blocks_t[occ_first[pair] % orbs]
        parts_out[turn, i, step] = dot(left, blocks[second_at[pair]]).astype(bf16)

    def integrals(turn):
        arrivals = window.at[turn, pl.ds(0, len(places) * orbs)]
        whole(arrivals, win_send.at[turn], win_recv.at[turn]).wait_recv()
        for at in range(SIDES * orbs):
            blocks[at] = window[turn, at]

        def one(i):
            for step in range(ranks - 1, -1, -1):
                integral(turn, step, i)
                if step > 0 and not square:
                    part_copy(turn, step, i).start()

        if square:
            for i in range(own_pairs):
                integral(turn, 3, i)
            for i in range(own_pairs):
                for step in (2, 1, 0):
                    integral(turn, step, i)
        else:
            pl.loop(0, own_pairs)(one)

    def far_sums(turn):
        def direct():
            for i in range(own_pairs):
                for step in (3, 1, 2):
                    part_copy(turn, step, i).start()

        def relays():
            for i in range(own_pairs):
                part_relay(turn, i).start()

        either(kinds(SUM_DIRECT, turn), direct, relays)

    def near_sums(turn):
        def relays():
            for i in range(own_pairs):
                part_copy(turn, 1 if i % 2 == 0 else 2, i).start()

        either(kinds(SUM_DIRECT, turn), nothing, relays)

    def through(turn, step):
        base = source(step) * own_pairs
        halves = []
        for i in range(own_pairs):
            amp = amps[turn, base + i]
            amps_now[base + i] = amp
            halves.append(dot(maps[base + i, 1], amp).astype(bf16))
        wholes = [dot(halves[i], first_t[base + i]) for i in range(own_pairs)]
        for i in range(own_pairs):
            local = occ_first[base + i] % orbs
            rows = pl.ds((step * own_pairs + i) * virtuals, virtuals)
            for o in range(orbs):
                masked = jnp.where(local == o, wholes[i], 0.0).astype(bf16)
                weights[rows, o * virtuals : (o + 1) * virtuals] = masked

    def applied(turn, some):
        lefts = [
            blocks[second_at[source(step) * own_pairs + i]]
            for step in some
            for i in range(own_pairs)
        ]
        rows = own_pairs * virtuals
        right = weights[pl.ds(some[0] * rows, len(some) * rows), :]
        return dot(jnp.concatenate(lefts, axis=1), right)

    def fit_near(turn):
        fitted[...] = applied(turn, near_steps)

    def dress(turn):
        if square:
            total = fitted[...] + applied(turn, far_steps)
        else:

            @pl.loop(1, ranks)
            def _(step):
                fitted[...] += applied(turn, (step,))

            total = fitted[...]
        values = [
            window[0, REACH * orbs + o].astype(jnp.float32)
            + dress_scale * total[:, o * virtuals : (o + 1) * virtuals]
            for o in range(orbs)
        ]

        @pl.when(turn + 1 < ITERS)
        def _():
            for o in range(orbs):
                window[turn + 1, REACH * orbs + o] = values[o].astype(bf16)

        @pl.when(turn + 1 == ITERS)
        def _():
            for o in range(orbs):
                out_dressed[o] = values[o]

    def couplings(turn):
        def one(i):
            halves = [
                dot(inter[i, k], amps_now[couple[i, k] % pairs]).astype(bf16)
                for k in range(partners)
            ]
            coupled[i] = dot(jnp.concatenate(halves, axis=1), inter_t[i])

        for i in range(own_pairs):
            one(i)

    def finish(turn):
        for first in range(0, own_pairs, BATCH):
            batch = range(first, min(first + BATCH, own_pairs))
            part_wait(turn, first // BATCH)
            totals = {}
            for i in batch:
                total = parts_out[turn, i, 0].astype(jnp.float32)
                for step in range(1, ranks if SUM_DIRECT != NONE or not square else 3):
                    total += parts_in[turn, i // BATCH, step - 1, i % BATCH].astype(jnp.float32)
                totals[i] = total.astype(bf16)
            rights = {i: dot(totals[i], maps[own + i, 1]).astype(bf16) for i in batch}
            values = {
                i: (dot(first_t[own + i], rights[i]) + coupled[i]) * scale[i] for i in batch
            }

            @pl.when(turn + 1 < ITERS)
            def _(batch=batch, values=values):
                for i in batch:
                    amps[turn + 1, own + i] = values[i].astype(bf16)
                amps_start(turn + 1, batch)

            @pl.when(turn + 1 == ITERS)
            def _(batch=batch, values=values):
                for i in batch:
                    out_amps[i] = values[i]

    win_start(0, True)
    orb_copy = pltpu.make_async_copy(orb_hbm, window.at[0, middle], orb_sem)
    orb_copy.start()
    small_copies[0].wait()
    for i in range(own_pairs):
        amps[0, own + i] = amplitudes[i].astype(bf16)
    amps_start(0, range(own_pairs))
    for copy in small_copies[1:]:
        copy.start()
    maps_copy = pltpu.make_async_copy(maps_hbm, maps, maps_sem)
    maps_copy.start()
    inter_copy = pltpu.make_async_copy(inter_hbm, inter, inter_sem)
    inter_copy.start()

    for copy in small_copies[1:]:
        copy.wait()

    @pl.loop(0, pairs)
    def _(pair):
        second = occ_second[pair]
        distance = (second // orbs - group + REACH + groups) % groups
        second_at[pair] = jnp.minimum(distance, SIDES - 1) * orbs + second % orbs

    if square and SUM_DIRECT != NONE:
        for turn in range(ITERS):

            def zero(turn=turn):
                for i in range(own_pairs):
                    parts_in[turn, i // BATCH, 2, i % BATCH] = jnp.zeros((size, size), bf16)

            either(kinds(SUM_DIRECT, turn), nothing, zero)

    orb_copy.wait()
    transposed(0)
    maps_copy.wait()

    @pl.loop(0, ranks)
    def _(block):
        for i in range(own_pairs):
            first_t[block * own_pairs + i] = maps[block * own_pairs + i, 0].T

    inter_copy.wait()

    @pl.loop(0, own_pairs)
    def _(i):
        rows = jnp.broadcast_to(pno_energy[pl.ds(i, 1), :], (size, size))
        denominator = rows + rows.T
        denominator -= occ_energy[occ_first[own + i]]
        denominator -= occ_energy[occ_second[own + i]]
        scale[i] = -1.0 / denominator
        for k in range(partners):
            inter_t[i, k * size : (k + 1) * size, :] = inter[i, k].T

    near_steps = (0, 1, 2) if square else (0,)
    far_steps = (3,) if square else tuple(range(1, ranks))

    def throughs(turn, some):
        first, last = some[0], some[-1] + 1
        if square and first > 0:
            amp_wait(turn, own_pairs + (0 if first == 1 else 1))

        @pl.loop(first, last)
        def _(step):
            if not square and first > 0:
                amp_wait(turn, step)
            through(turn, step)

    near_steps = (0, 1, 2) if square else (0,)
    far_steps = (3,) if square else tuple(range(1, ranks))
    throughs(0, (0,))
    relay_first = {"all": True, "inner": inner, "none": False}[FIRST_RELAY]
    if square:
        either(relay_first, lambda: relay_all(0), nothing)
        if EARLY_NEAR:
            either(inner, lambda: throughs(0, (1, 2)), nothing)

    def sums(turn, place):
        def some(far_place, near_place):
            if far_place == place:
                far_sums(turn)
            if near_place == place:
                near_sums(turn)

        either(inner, lambda: some(INNER_FAR, INNER_NEAR), lambda: some(0, 1))

    @pl.loop(0, ITERS)
    def _(turn):
        integrals(turn)

        if square:

            @pl.when(turn == 0)
            def _():
                far_sums(turn)
                if NEAR_AT == 0:
                    near_sums(turn)

            @pl.when(turn > 0)
            def _():
                sums(turn, 0)
                throughs(turn, (0,))
                relay_all(turn)
                sums(turn, 1)

            if EARLY_NEAR:

                @pl.when(jnp.logical_or(turn > 0, jnp.logical_not(inner)))
                def _():
                    throughs(turn, (1, 2))

            else:
                throughs(turn, (1, 2))
        else:

            @pl.when(turn > 0)
            def _():
                throughs(turn, (0,))

        fit_near(turn)
        if square:

            @pl.when(turn > 0)
            def _():
                sums(turn, 2)
                either(inner, nothing, lambda: forward_all(turn))

        throughs(turn, far_steps)
        dress(turn)

        @pl.when(turn + 1 < ITERS)
        def _():
            win_start(turn + 1)
            if square:
                if NEAR_AT == 1:
                    near_sums(turn)
                forward_all(turn)
                if NEAR_AT == 2:
                    near_sums(turn)
            transposed(turn + 1)

        if square:

            @pl.when(jnp.logical_and(turn > 0, inner))
            def _():
                forward_all(turn)

        couplings(turn)

        @pl.when(turn > 0)
        def _():
            sent(turn - 1)
            parts_sent(turn - 1)

        finish(turn)

    sent(ITERS - 1)
    parts_sent(ITERS - 1)


def store(amps, dressed, out_amps, out_dressed, sem):
    copies = [
        pltpu.make_async_copy(amps, out_amps, sem.at[0]),
        pltpu.make_async_copy(dressed, out_dressed, sem.at[1]),
    ]
    for copy in copies:
        copy.start()
    for copy in copies:
        copy.wait()


def on_device(
    ranks,
    groups,
    amplitudes,
    couple,
    occ_first,
    occ_second,
    couple_intersection,
    pno_maps,
    orbital_blocks,
    pno_energy,
    occ_energy,
):
    own_pairs, size, _ = amplitudes.shape
    group_pairs = occ_first.shape[0]
    orbs, rows, virtuals = orbital_blocks.shape
    partners = couple.shape[1]
    bf16 = jnp.bfloat16
    vmem = pl.BlockSpec(memory_space=pltpu.VMEM)
    hbm = pl.BlockSpec(memory_space=pltpu.HBM)
    dma = pltpu.SemaphoreType.DMA
    square = ranks == 4 and own_pairs % BATCH == 0
    results = pl.pallas_call(
        functools.partial(kernel, ranks, groups),
        out_shape=(
            pltpu.VMEM(amplitudes.shape, jnp.float32),
            pltpu.VMEM(orbital_blocks.shape, jnp.float32),
        ),
        in_specs=[hbm] * 9,
        out_specs=(vmem, vmem),
        scratch_shapes=[
            pltpu.SMEM(couple.shape, couple.dtype),
            pltpu.SMEM(occ_first.shape, occ_first.dtype),
            pltpu.SMEM(occ_second.shape, occ_second.dtype),
            pltpu.SMEM(occ_energy.shape, occ_energy.dtype),
            pltpu.SMEM(occ_second.shape, occ_second.dtype),
            pltpu.VMEM(amplitudes.shape, amplitudes.dtype),
            pltpu.VMEM(pno_energy.shape, pno_energy.dtype),
            pltpu.VMEM(couple_intersection.shape, bf16),
            pltpu.VMEM((own_pairs, partners * size, size), bf16),
            pltpu.VMEM(pno_maps.shape, bf16),
            pltpu.VMEM((group_pairs, size, virtuals), bf16),
            pltpu.VMEM((orbs, virtuals, rows), bf16),
            pltpu.VMEM((own_pairs, size, size), jnp.float32),
            pltpu.VMEM((own_pairs, size, size), jnp.float32),
            pltpu.VMEM((ITERS, group_pairs, size, size), bf16),
            pltpu.VMEM((group_pairs, size, size), bf16),
            pltpu.VMEM((ITERS, SIDES * orbs, rows, virtuals), bf16),
            pltpu.VMEM((SIDES * orbs, rows, virtuals), bf16),
            pltpu.VMEM((ITERS, own_pairs, ranks, virtuals, virtuals), bf16),
            pltpu.VMEM((ITERS, own_pairs // BATCH, ranks - 1, BATCH, virtuals, virtuals), bf16),
            pltpu.VMEM((ITERS, own_pairs, virtuals, virtuals), bf16),
            pltpu.VMEM((group_pairs * virtuals, orbs * virtuals), bf16),
            pltpu.VMEM((rows, orbs * virtuals), jnp.float32),
            dma((ITERS,)),
            dma((ITERS, own_pairs + 2 if square else ranks)),
            dma((ITERS,)),
            dma((ITERS,)),
            dma((ITERS,)),
            dma((ITERS, own_pairs // BATCH)),
            dma((ITERS, own_pairs // BATCH)),
            dma,
            dma,
            dma,
            dma((6,)),
        ],
        compiler_params=pltpu.CompilerParams(
            collective_id=0, has_side_effects=True, vmem_limit_bytes=67043328 - 4096 * 1024
        ),
    )(
        *(pltpu.with_memory_space_constraint(x, pltpu.HBM) for x in (
        couple,
        occ_first,
        occ_second,
        occ_energy,
        amplitudes,
        pno_energy,
        couple_intersection,
        pno_maps,
        orbital_blocks,
        ))
    )
    return pl.pallas_call(
        store,
        out_shape=tuple(pltpu.HBM(x.shape, x.dtype) for x in results),
        in_specs=[vmem] * 2,
        out_specs=(hbm, hbm),
        scratch_shapes=[dma((2,))],
        compiler_params=pltpu.CompilerParams(vmem_limit_bytes=4096 * 1024),
    )(*(pltpu.with_memory_space_constraint(x, pltpu.VMEM) for x in results))


def solution(mesh):
    return jax.shard_map(
        functools.partial(on_device, mesh.shape["orb"], mesh.shape["pair"]),
        mesh=mesh,
        in_specs=(
            P(("pair", "orb"), None, None),
            P(("pair", "orb"), None),
            P("pair"),
            P("pair"),
            P(("pair", "orb"), None, None, None),
            P("pair", None, None, None),
            P("pair", "orb", None),
            P(("pair", "orb"), None),
            P(),
        ),
        out_specs=(P(("pair", "orb"), None, None), P("pair", "orb", None)),
        check_vma=False,
    )
```

```python
import functools

import jax
import jax.numpy as jnp
from jax import lax
from jax.experimental import pallas as pl
from jax.experimental.pallas import tpu as pltpu
from jax.sharding import PartitionSpec as P

REACH = 1
ITERS = 2
SIDES = 2 * REACH + 1

dress_scale = 0.015
BATCH = 2
SUM_DIRECT = ("outer", "none")
NONE = ("none", "none")
FIRST_RELAY = "all"
EARLY_NEAR = True
NEAR_AT = 0
INNER_FAR = 1
INNER_NEAR = 2

NN = (((1,), (0,)), ((), ()))
NT = (((1,), (1,)), ((), ()))


def dot(left, right, dims=NN):
    return lax.dot_general(left, right, dims, preferred_element_type=jnp.float32)


def kernel(
    ranks,
    groups,
    couple_hbm,
    first_hbm,
    second_hbm,
    energy_hbm,
    amps_hbm,
    pno_hbm,
    inter_hbm,
    maps_hbm,
    orb_hbm,
    out_amps,
    out_dressed,
    couple,
    occ_first,
    occ_second,
    occ_energy,
    second_at,
    amplitudes,
    pno_energy,
    inter,
    inter_t,
    maps,
    first_t,
    blocks_t,
    scale,
    coupled,
    amps,
    amps_now,
    window,
    blocks,
    parts_out,
    parts_in,
    relayed,
    weights,
    fitted,
    amp_send,
    amp_recv,
    win_send,
    win_recv,
    part_send,
    part_recv,
    relay_recv,
):
    own_pairs = amps_hbm.shape[0]
    orbs = orb_hbm.shape[0]
    partners = couple.shape[1]
    size = amplitudes.shape[2]
    virtuals = orb_hbm.shape[2]
    pairs = ranks * own_pairs
    me = lax.axis_index("orb")
    group = lax.axis_index("pair")
    own = me * own_pairs
    middle = pl.ds(REACH * orbs, orbs)
    places = [place for place in range(SIDES) if place != REACH]
    bf16 = jnp.bfloat16
    square = ranks == 4 and own_pairs % BATCH == 0
    z_place = (group + 1) % 2 * 2 * REACH
    c_place = 2 * REACH - z_place

    def target(step):
        if square:
            return (me // 2 + step // 2) % 2 * 2 + (me + step) % 2
        return (me + step) % ranks

    def source(step):
        return target(step) if square else (me + ranks - step) % ranks

    inner = group % 2 == 1

    def kinds(modes, turn):
        flags = [{"none": False, "all": True, "outer": jnp.logical_not(inner)}[m] for m in modes]
        if isinstance(turn, int):
            return flags[turn]
        if all(mode == modes[0] for mode in modes):
            return flags[0]
        flag = False
        for at in range(ITERS):
            flag = jnp.logical_or(flag, jnp.logical_and(turn == at, flags[at]))
        return flag

    def either(flag, yes, no):
        if isinstance(flag, bool):
            (yes if flag else no)()
        else:
            pl.when(flag)(yes)
            pl.when(jnp.logical_not(flag))(no)

    def nothing():
        pass

    barrier = pltpu.get_barrier_semaphore()
    for step in range(1, ranks):
        pl.semaphore_signal(
            barrier,
            inc=1,
            device_id={"orb": (me + step) % ranks},
            device_id_type=pl.DeviceIdType.MESH,
        )
    for step in range(1, REACH + 1):
        for shift in (step, groups - step):
            pl.semaphore_signal(
                barrier,
                inc=1,
                device_id={"pair": (group + shift) % groups},
                device_id_type=pl.DeviceIdType.MESH,
            )

    small_copies = [
        pltpu.make_async_copy(source_ref, target_ref, amp_recv.at[ITERS - 1, at])
        for at, (source_ref, target_ref) in enumerate(
            (
                (amps_hbm, amplitudes),
                (first_hbm, occ_first),
                (second_hbm, occ_second),
                (energy_hbm, occ_energy),
                (pno_hbm, pno_energy),
                (couple_hbm, couple),
            )
        )
    ]
    small_copies[0].start()
    pl.semaphore_wait(barrier, ranks - 1 + 2 * REACH)

    def win_copy(turn, place, bare=False):
        return pltpu.make_async_remote_copy(
            src_ref=orb_hbm if bare else window.at[turn, middle],
            dst_ref=window.at[turn, pl.ds(place * orbs, orbs)],
            send_sem=win_send.at[turn],
            recv_sem=win_recv.at[turn],
            device_id={"pair": (group + REACH - place + groups) % groups},
            device_id_type=pl.DeviceIdType.MESH,
        )

    def relayed_tile(step, i):
        return (step, i % 2) in ((1, 0), (2, 1))

    def amp_slot(step, i):
        if not square:
            return step
        return i if relayed_tile(step, i) else own_pairs

    def amp_copy(turn, step, i):
        return pltpu.make_async_remote_copy(
            src_ref=amps.at[turn, own + i],
            dst_ref=amps.at[turn, own + i],
            send_sem=amp_send.at[turn],
            recv_sem=amp_recv.at[turn, amp_slot(step, i)],
            device_id={"orb": target(step)},
            device_id_type=pl.DeviceIdType.MESH,
        )

    def amp_relay(turn, i):
        via, onto = (1, 2) if i % 2 == 0 else (2, 1)
        place = target(via) * own_pairs + i
        return pltpu.make_async_remote_copy(
            src_ref=amps.at[turn, place],
            dst_ref=amps.at[turn, place],
            send_sem=amp_send.at[turn],
            recv_sem=amp_recv.at[turn, own_pairs + 1],
            device_id={"orb": target(onto)},
            device_id_type=pl.DeviceIdType.MESH,
        )

    def relay_all(turn):
        for i in range(own_pairs):
            amp_copy(turn, 1 if i % 2 == 0 else 2, i).wait_recv()
            amp_relay(turn, i).start()

    def amp_wait(turn, slot):
        block = amps.at[turn, pl.ds(own, own_pairs)]
        whole(block, amp_send.at[turn], amp_recv.at[turn, slot]).wait_recv()

    def part_copy(turn, step, i):
        return pltpu.make_async_remote_copy(
            src_ref=parts_out.at[turn, i, step],
            dst_ref=parts_in.at[turn, i // BATCH, step - 1, i % BATCH],
            send_sem=part_send.at[turn],
            recv_sem=part_recv.at[turn, i // BATCH],
            device_id={"orb": target(step)},
            device_id_type=pl.DeviceIdType.MESH,
        )

    def part_relay(turn, i):
        return pltpu.make_async_remote_copy(
            src_ref=parts_out.at[turn, i, 3],
            dst_ref=relayed.at[turn, i],
            send_sem=part_send.at[turn],
            recv_sem=relay_recv.at[turn, i // BATCH],
            device_id={"orb": target(1 if i % 2 == 0 else 2)},
            device_id_type=pl.DeviceIdType.MESH,
        )

    def forward_all(turn):
        def relays():
            for first in range(0, own_pairs, BATCH):
                arrived = relayed.at[turn, pl.ds(first, BATCH)]
                whole(arrived, part_send.at[turn], relay_recv.at[turn, first // BATCH]).wait_recv()
                for i in range(first, first + BATCH):
                    onto = 2 if i % 2 == 0 else 1
                    total = parts_out[turn, i, onto].astype(jnp.float32)
                    total += relayed[turn, i].astype(jnp.float32)
                    parts_out[turn, i, onto] = total.astype(bf16)
                for i in range(first, first + BATCH):
                    part_copy(turn, 2 if i % 2 == 0 else 1, i).start()

        either(kinds(SUM_DIRECT, turn), nothing, relays)

    def whole(ref, send_sem, recv_sem):
        return pltpu.make_async_remote_copy(
            src_ref=ref,
            dst_ref=ref,
            send_sem=send_sem,
            recv_sem=recv_sem,
            device_id={"orb": target(1)},
            device_id_type=pl.DeviceIdType.MESH,
        )

    def part_wait(turn, at):
        def wait(terms):
            arrived = parts_in.at[turn, at, pl.ds(0, terms)]
            whole(arrived, part_send.at[turn], part_recv.at[turn, at]).wait_recv()

        if square:
            either(kinds(SUM_DIRECT, turn), lambda: wait(3), lambda: wait(2))
        else:
            wait(ranks - 1)

    def sent(turn):
        sends = pl.ds(0, (ranks - 1) * own_pairs)
        whole(amps.at[turn, sends], amp_send.at[turn], amp_recv.at[turn, 0]).wait_send()
        sends = pl.ds(0, len(places) * orbs)
        whole(window.at[turn, sends], win_send.at[turn], win_recv.at[turn]).wait_send()

    def parts_sent(turn):
        whole(parts_in.at[turn], part_send.at[turn], part_recv.at[turn, 0]).wait_send()

    def amp_start(turn, i):
        for step in range(ranks - 1, 0, -1):
            amp_copy(turn, step, i).start()

    def amps_start(turn, batch):
        if square:
            for turned in (0, 1):
                for i in batch:
                    amp_copy(turn, 1 if (i + turned) % 2 == 0 else 2, i).start()
        else:
            for i in batch:
                amp_start(turn, i)

    def win_start(turn, bare=False):
        win_copy(turn, c_place, bare).start()
        win_copy(turn, z_place, bare).start()

    def transposed(turn):
        for o in range(orbs):
            blocks_t[o] = window[turn, REACH * orbs + o].T

    def integral(turn, step, i):
        pair = target(step) * own_pairs + i
        left = blocks_t[occ_first[pair] % orbs]
        parts_out[turn, i, step] = dot(left, blocks[second_at[pair]]).astype(bf16)

    def integrals(turn):
        arrivals = window.at[turn, pl.ds(0, len(places) * orbs)]
        whole(arrivals, win_send.at[turn], win_recv.at[turn]).wait_recv()
        for at in range(SIDES * orbs):
            blocks[at] = window[turn, at]

        def one(i):
            for step in range(ranks - 1, -1, -1):
                integral(turn, step, i)
                if step > 0 and not square:
                    part_copy(turn, step, i).start()

        if square:
            for i in range(own_pairs):
                integral(turn, 3, i)
            for i in range(own_pairs):
                for step in (2, 1, 0):
                    integral(turn, step, i)
        else:
            pl.loop(0, own_pairs)(one)

    def far_sums(turn):
        def direct():
            for i in range(own_pairs):
                for step in (3, 1, 2):
                    part_copy(turn, step, i).start()

        def relays():
            for i in range(own_pairs):
                part_relay(turn, i).start()

        either(kinds(SUM_DIRECT, turn), direct, relays)

    def near_sums(turn):
        def relays():
            for i in range(own_pairs):
                part_copy(turn, 1 if i % 2 == 0 else 2, i).start()

        either(kinds(SUM_DIRECT, turn), nothing, relays)

    def through(turn, step):
        base = source(step) * own_pairs
        halves = []
        for i in range(own_pairs):
            amp = amps[turn, base + i]
            amps_now[base + i] = amp
            halves.append(dot(maps[base + i, 1], amp).astype(bf16))
        wholes = [dot(halves[i], first_t[base + i]) for i in range(own_pairs)]
        for i in range(own_pairs):
            local = occ_first[base + i] % orbs
            rows = pl.ds((step * own_pairs + i) * virtuals, virtuals)
            for o in range(orbs):
                masked = jnp.where(local == o, wholes[i], 0.0).astype(bf16)
                weights[rows, o * virtuals : (o + 1) * virtuals] = masked

    def applied(turn, some):
        lefts = [
            blocks[second_at[source(step) * own_pairs + i]]
            for step in some
            for i in range(own_pairs)
        ]
        rows = own_pairs * virtuals
        right = weights[pl.ds(some[0] * rows, len(some) * rows), :]
        return dot(jnp.concatenate(lefts, axis=1), right)

    def fit_near(turn):
        fitted[...] = applied(turn, near_steps)

    def dress(turn):
        if square:
            total = fitted[...] + applied(turn, far_steps)
        else:

            @pl.loop(1, ranks)
            def _(step):
                fitted[...] += applied(turn, (step,))

            total = fitted[...]
        values = [
            window[0, REACH * orbs + o].astype(jnp.float32)
            + dress_scale * total[:, o * virtuals : (o + 1) * virtuals]
            for o in range(orbs)
        ]

        @pl.when(turn + 1 < ITERS)
        def _():
            for o in range(orbs):
                window[turn + 1, REACH * orbs + o] = values[o].astype(bf16)

        @pl.when(turn + 1 == ITERS)
        def _():
            for o in range(orbs):
                out_dressed[o] = values[o]

    def couplings(turn):
        def one(i):
            halves = [
                dot(inter[i, k], amps_now[couple[i, k] % pairs]).astype(bf16)
                for k in range(partners)
            ]
            coupled[i] = dot(jnp.concatenate(halves, axis=1), inter_t[i])

        for i in range(own_pairs):
            one(i)

    def finish(turn):
        for first in range(0, own_pairs, BATCH):
            batch = range(first, min(first + BATCH, own_pairs))
            part_wait(turn, first // BATCH)
            totals = {}
            for i in batch:
                total = parts_out[turn, i, 0].astype(jnp.float32)
                for step in range(1, ranks if SUM_DIRECT != NONE or not square else 3):
                    total += parts_in[turn, i // BATCH, step - 1, i % BATCH].astype(jnp.float32)
                totals[i] = total.astype(bf16)
            rights = {i: dot(totals[i], maps[own + i, 1]).astype(bf16) for i in batch}
            values = {
                i: (dot(first_t[own + i], rights[i]) + coupled[i]) * scale[i] for i in batch
            }

            @pl.when(turn + 1 < ITERS)
            def _(batch=batch, values=values):
                for i in batch:
                    amps[turn + 1, own + i] = values[i].astype(bf16)
                amps_start(turn + 1, batch)

            @pl.when(turn + 1 == ITERS)
            def _(batch=batch, values=values):
                for i in batch:
                    out_amps[i] = values[i]

    win_start(0, True)
    orb_copy = pltpu.make_async_copy(orb_hbm, window.at[0, middle], relay_recv.at[ITERS - 1, 0])
    orb_copy.start()
    small_copies[0].wait()
    for i in range(own_pairs):
        amps[0, own + i] = amplitudes[i].astype(bf16)
    amps_start(0, range(own_pairs))
    for copy in small_copies[1:]:
        copy.start()
    maps_copy = pltpu.make_async_copy(maps_hbm, maps, part_recv.at[ITERS - 1, 0])
    maps_copy.start()
    inter_copy = pltpu.make_async_copy(inter_hbm, inter, part_recv.at[ITERS - 1, 1])
    inter_copy.start()

    for copy in small_copies[1:]:
        copy.wait()

    @pl.loop(0, pairs)
    def _(pair):
        second = occ_second[pair]
        distance = (second // orbs - group + REACH + groups) % groups
        second_at[pair] = jnp.minimum(distance, SIDES - 1) * orbs + second % orbs

    if square and SUM_DIRECT != NONE:
        for turn in range(ITERS):

            def zero(turn=turn):
                for i in range(own_pairs):
                    parts_in[turn, i // BATCH, 2, i % BATCH] = jnp.zeros((size, size), bf16)

            either(kinds(SUM_DIRECT, turn), nothing, zero)

    orb_copy.wait()
    transposed(0)
    maps_copy.wait()

    @pl.loop(0, ranks)
    def _(block):
        for i in range(own_pairs):
            first_t[block * own_pairs + i] = maps[block * own_pairs + i, 0].T

    inter_copy.wait()

    @pl.loop(0, own_pairs)
    def _(i):
        rows = jnp.broadcast_to(pno_energy[pl.ds(i, 1), :], (size, size))
        denominator = rows + rows.T
        denominator -= occ_energy[occ_first[own + i]]
        denominator -= occ_energy[occ_second[own + i]]
        scale[i] = -1.0 / denominator
        for k in range(partners):
            inter_t[i, k * size : (k + 1) * size, :] = inter[i, k].T

    near_steps = (0, 1, 2) if square else (0,)
    far_steps = (3,) if square else tuple(range(1, ranks))

    def throughs(turn, some):
        first, last = some[0], some[-1] + 1
        if square and first > 0:
            amp_wait(turn, own_pairs + (0 if first == 1 else 1))

        @pl.loop(first, last)
        def _(step):
            if not square and first > 0:
                amp_wait(turn, step)
            through(turn, step)

    near_steps = (0, 1, 2) if square else (0,)
    far_steps = (3,) if square else tuple(range(1, ranks))
    throughs(0, (0,))
    relay_first = {"all": True, "inner": inner, "none": False}[FIRST_RELAY]
    if square:
        either(relay_first, lambda: relay_all(0), nothing)
        if EARLY_NEAR:
            either(inner, lambda: throughs(0, (1, 2)), nothing)

    def sums(turn, place):
        def some(far_place, near_place):
            if far_place == place:
                far_sums(turn)
            if near_place == place:
                near_sums(turn)

        either(inner, lambda: some(INNER_FAR, INNER_NEAR), lambda: some(0, 1))

    @pl.loop(0, ITERS)
    def _(turn):
        integrals(turn)

        if square:

            @pl.when(turn == 0)
            def _():
                far_sums(turn)
                if NEAR_AT == 0:
                    near_sums(turn)

            @pl.when(turn > 0)
            def _():
                sums(turn, 0)
                throughs(turn, (0,))
                relay_all(turn)
                sums(turn, 1)

            if EARLY_NEAR:

                @pl.when(jnp.logical_or(turn > 0, jnp.logical_not(inner)))
                def _():
                    throughs(turn, (1, 2))

            else:
                throughs(turn, (1, 2))
        else:

            @pl.when(turn > 0)
            def _():
                throughs(turn, (0,))

        fit_near(turn)
        if square:

            @pl.when(turn > 0)
            def _():
                sums(turn, 2)
                either(inner, nothing, lambda: forward_all(turn))

        throughs(turn, far_steps)
        dress(turn)

        @pl.when(turn + 1 < ITERS)
        def _():
            win_start(turn + 1)
            if square:
                if NEAR_AT == 1:
                    near_sums(turn)
                forward_all(turn)
                if NEAR_AT == 2:
                    near_sums(turn)
            transposed(turn + 1)

        if square:

            @pl.when(jnp.logical_and(turn > 0, inner))
            def _():
                forward_all(turn)

        couplings(turn)

        @pl.when(turn > 0)
        def _():
            sent(turn - 1)
            parts_sent(turn - 1)

        finish(turn)

    sent(ITERS - 1)
    parts_sent(ITERS - 1)


def store(amps, dressed, out_amps, out_dressed, sem):
    copies = [
        pltpu.make_async_copy(amps, out_amps, sem.at[0]),
        pltpu.make_async_copy(dressed, out_dressed, sem.at[1]),
    ]
    for copy in copies:
        copy.start()
    for copy in copies:
        copy.wait()


def on_device(
    ranks,
    groups,
    amplitudes,
    couple,
    occ_first,
    occ_second,
    couple_intersection,
    pno_maps,
    orbital_blocks,
    pno_energy,
    occ_energy,
):
    own_pairs, size, _ = amplitudes.shape
    group_pairs = occ_first.shape[0]
    orbs, rows, virtuals = orbital_blocks.shape
    partners = couple.shape[1]
    bf16 = jnp.bfloat16
    vmem = pl.BlockSpec(memory_space=pltpu.VMEM)
    hbm = pl.BlockSpec(memory_space=pltpu.HBM)
    dma = pltpu.SemaphoreType.DMA
    square = ranks == 4 and own_pairs % BATCH == 0
    results = pl.pallas_call(
        functools.partial(kernel, ranks, groups),
        out_shape=(
            pltpu.VMEM(amplitudes.shape, jnp.float32),
            pltpu.VMEM(orbital_blocks.shape, jnp.float32),
        ),
        in_specs=[hbm] * 9,
        out_specs=(vmem, vmem),
        scratch_shapes=[
            pltpu.SMEM(couple.shape, couple.dtype),
            pltpu.SMEM(occ_first.shape, occ_first.dtype),
            pltpu.SMEM(occ_second.shape, occ_second.dtype),
            pltpu.SMEM(occ_energy.shape, occ_energy.dtype),
            pltpu.SMEM(occ_second.shape, occ_second.dtype),
            pltpu.VMEM(amplitudes.shape, amplitudes.dtype),
            pltpu.VMEM(pno_energy.shape, pno_energy.dtype),
            pltpu.VMEM(couple_intersection.shape, bf16),
            pltpu.VMEM((own_pairs, partners * size, size), bf16),
            pltpu.VMEM(pno_maps.shape, bf16),
            pltpu.VMEM((group_pairs, size, virtuals), bf16),
            pltpu.VMEM((orbs, virtuals, rows), bf16),
            pltpu.VMEM((own_pairs, size, size), jnp.float32),
            pltpu.VMEM((own_pairs, size, size), jnp.float32),
            pltpu.VMEM((ITERS, group_pairs, size, size), bf16),
            pltpu.VMEM((group_pairs, size, size), bf16),
            pltpu.VMEM((ITERS, SIDES * orbs, rows, virtuals), bf16),
            pltpu.VMEM((SIDES * orbs, rows, virtuals), bf16),
            pltpu.VMEM((ITERS, own_pairs, ranks, virtuals, virtuals), bf16),
            pltpu.VMEM((ITERS, own_pairs // BATCH, ranks - 1, BATCH, virtuals, virtuals), bf16),
            pltpu.VMEM((ITERS, own_pairs, virtuals, virtuals), bf16),
            pltpu.VMEM((group_pairs * virtuals, orbs * virtuals), bf16),
            pltpu.VMEM((rows, orbs * virtuals), jnp.float32),
            dma((ITERS,)),
            dma((ITERS, own_pairs + 2 if square else ranks)),
            dma((ITERS,)),
            dma((ITERS,)),
            dma((ITERS,)),
            dma((ITERS, own_pairs // BATCH)),
            dma((ITERS, own_pairs // BATCH)),
        ],
        compiler_params=pltpu.CompilerParams(
            collective_id=0, has_side_effects=True, vmem_limit_bytes=67043328 - 4096 * 1024
        ),
    )(
        *(pltpu.with_memory_space_constraint(x, pltpu.HBM) for x in (
        couple,
        occ_first,
        occ_second,
        occ_energy,
        amplitudes,
        pno_energy,
        couple_intersection,
        pno_maps,
        orbital_blocks,
        ))
    )
    return pl.pallas_call(
        store,
        out_shape=tuple(pltpu.HBM(x.shape, x.dtype) for x in results),
        in_specs=[vmem] * 2,
        out_specs=(hbm, hbm),
        scratch_shapes=[dma((2,))],
        compiler_params=pltpu.CompilerParams(vmem_limit_bytes=4096 * 1024),
    )(*(pltpu.with_memory_space_constraint(x, pltpu.VMEM) for x in results))


def solution(mesh):
    return jax.shard_map(
        functools.partial(on_device, mesh.shape["orb"], mesh.shape["pair"]),
        mesh=mesh,
        in_specs=(
            P(("pair", "orb"), None, None),
            P(("pair", "orb"), None),
            P("pair"),
            P("pair"),
            P(("pair", "orb"), None, None, None),
            P("pair", None, None, None),
            P("pair", "orb", None),
            P(("pair", "orb"), None),
            P(),
        ),
        out_specs=(P(("pair", "orb"), None, None), P("pair", "orb", None)),
        check_vma=False,
    )
```

```python
import functools

import jax
import jax.numpy as jnp
from jax import lax
from jax.experimental import pallas as pl
from jax.experimental.pallas import tpu as pltpu
from jax.sharding import PartitionSpec as P

REACH = 1
ITERS = 2
SIDES = 2 * REACH + 1

dress_scale = 0.015
BATCH = 2
GATHER_FAR = "none"
FORWARD_EARLY = False
SUM_DIRECT = ("outer", "none")
NONE = ("none", "none")
FIRST_RELAY = "all"
EARLY_NEAR = True
NEAR_AT = 0
INNER_FAR = 1
INNER_NEAR = 2

NN = (((1,), (0,)), ((), ()))
NT = (((1,), (1,)), ((), ()))


def dot(left, right, dims=NN):
    return lax.dot_general(left, right, dims, preferred_element_type=jnp.float32)


def kernel(
    ranks,
    groups,
    couple_hbm,
    first_hbm,
    second_hbm,
    energy_hbm,
    amps_hbm,
    pno_hbm,
    inter_hbm,
    maps_hbm,
    orb_hbm,
    out_amps,
    out_dressed,
    couple,
    occ_first,
    occ_second,
    occ_energy,
    second_at,
    amplitudes,
    pno_energy,
    inter,
    inter_t,
    maps,
    first_t,
    blocks_t,
    scale,
    coupled,
    amps,
    amps_now,
    window,
    blocks,
    parts_out,
    parts_in,
    relayed,
    weights,
    fitted,
    amp_send,
    amp_recv,
    win_send,
    win_recv,
    part_send,
    part_recv,
    relay_recv,
    inter_sem,
    maps_sem,
    orb_sem,
    small_sem,
):
    own_pairs = amps_hbm.shape[0]
    orbs = orb_hbm.shape[0]
    partners = couple.shape[1]
    size = amplitudes.shape[2]
    virtuals = orb_hbm.shape[2]
    pairs = ranks * own_pairs
    me = lax.axis_index("orb")
    group = lax.axis_index("pair")
    own = me * own_pairs
    middle = pl.ds(REACH * orbs, orbs)
    places = [place for place in range(SIDES) if place != REACH]
    bf16 = jnp.bfloat16
    square = ranks == 4 and own_pairs % BATCH == 0
    z_place = (group + 1) % 2 * 2 * REACH
    c_place = 2 * REACH - z_place

    def target(step):
        if square:
            return (me // 2 + step // 2) % 2 * 2 + (me + step) % 2
        return (me + step) % ranks

    def source(step):
        return target(step) if square else (me + ranks - step) % ranks

    inner = group % 2 == 1

    def kinds(modes, turn):
        flags = [{"none": False, "all": True, "outer": jnp.logical_not(inner)}[m] for m in modes]
        if isinstance(turn, int):
            return flags[turn]
        if all(mode == modes[0] for mode in modes):
            return flags[0]
        flag = False
        for at in range(ITERS):
            flag = jnp.logical_or(flag, jnp.logical_and(turn == at, flags[at]))
        return flag

    def either(flag, yes, no):
        if isinstance(flag, bool):
            (yes if flag else no)()
        else:
            pl.when(flag)(yes)
            pl.when(jnp.logical_not(flag))(no)

    def nothing():
        pass

    barrier = pltpu.get_barrier_semaphore()
    for step in range(1, ranks):
        pl.semaphore_signal(
            barrier,
            inc=1,
            device_id={"orb": (me + step) % ranks},
            device_id_type=pl.DeviceIdType.MESH,
        )
    for step in range(1, REACH + 1):
        for shift in (step, groups - step):
            pl.semaphore_signal(
                barrier,
                inc=1,
                device_id={"pair": (group + shift) % groups},
                device_id_type=pl.DeviceIdType.MESH,
            )

    small_copies = [
        pltpu.make_async_copy(source_ref, target_ref, small_sem.at[at])
        for at, (source_ref, target_ref) in enumerate(
            (
                (amps_hbm, amplitudes),
                (first_hbm, occ_first),
                (second_hbm, occ_second),
                (energy_hbm, occ_energy),
                (pno_hbm, pno_energy),
                (couple_hbm, couple),
            )
        )
    ]
    small_copies[0].start()
    pl.semaphore_wait(barrier, ranks - 1 + 2 * REACH)

    def win_copy(turn, place, bare=False):
        return pltpu.make_async_remote_copy(
            src_ref=orb_hbm if bare else window.at[turn, middle],
            dst_ref=window.at[turn, pl.ds(place * orbs, orbs)],
            send_sem=win_send.at[turn],
            recv_sem=win_recv.at[turn],
            device_id={"pair": (group + REACH - place + groups) % groups},
            device_id_type=pl.DeviceIdType.MESH,
        )

    def relayed_tile(step, i):
        return (step, i % 2) in ((1, 0), (2, 1))

    def amp_slot(step, i):
        if not square:
            return step
        if step == 3:
            return own_pairs + 1
        return i if relayed_tile(step, i) else own_pairs

    def amp_copy(turn, step, i):
        return pltpu.make_async_remote_copy(
            src_ref=amps.at[turn, own + i],
            dst_ref=amps.at[turn, own + i],
            send_sem=amp_send.at[turn],
            recv_sem=amp_recv.at[turn, amp_slot(step, i)],
            device_id={"orb": target(step)},
            device_id_type=pl.DeviceIdType.MESH,
        )

    def amp_relay(turn, i):
        via, onto = (1, 2) if i % 2 == 0 else (2, 1)
        place = target(via) * own_pairs + i
        return pltpu.make_async_remote_copy(
            src_ref=amps.at[turn, place],
            dst_ref=amps.at[turn, place],
            send_sem=amp_send.at[turn],
            recv_sem=amp_recv.at[turn, own_pairs + 1],
            device_id={"orb": target(onto)},
            device_id_type=pl.DeviceIdType.MESH,
        )

    def relay_some(turn, some):
        for i in some:
            amp_copy(turn, 1 if i % 2 == 0 else 2, i).wait_recv()
            amp_relay(turn, i).start()

    def relay_all(turn):
        relay_some(turn, range(own_pairs))

    beyond = range(BATCH, own_pairs)
    direct_far = {"all": True, "outer": jnp.logical_not(inner), "none": False}[GATHER_FAR]

    def amp_wait(turn, slot):
        block = amps.at[turn, pl.ds(own, own_pairs)]
        whole(block, amp_send.at[turn], amp_recv.at[turn, slot]).wait_recv()

    def part_copy(turn, step, i):
        return pltpu.make_async_remote_copy(
            src_ref=parts_out.at[turn, i, step],
            dst_ref=parts_in.at[turn, i // BATCH, step - 1, i % BATCH],
            send_sem=part_send.at[turn],
            recv_sem=part_recv.at[turn, i // BATCH],
            device_id={"orb": target(step)},
            device_id_type=pl.DeviceIdType.MESH,
        )

    def part_relay(turn, i):
        return pltpu.make_async_remote_copy(
            src_ref=parts_out.at[turn, i, 3],
            dst_ref=relayed.at[turn, i],
            send_sem=part_send.at[turn],
            recv_sem=relay_recv.at[turn, i // BATCH],
            device_id={"orb": target(1 if i % 2 == 0 else 2)},
            device_id_type=pl.DeviceIdType.MESH,
        )

    def forward_all(turn):
        def relays():
            for first in range(0, own_pairs, BATCH):
                arrived = relayed.at[turn, pl.ds(first, BATCH)]
                whole(arrived, part_send.at[turn], relay_recv.at[turn, first // BATCH]).wait_recv()
                for i in range(first, first + BATCH):
                    onto = 2 if i % 2 == 0 else 1
                    total = parts_out[turn, i, onto].astype(jnp.float32)
                    total += relayed[turn, i].astype(jnp.float32)
                    parts_out[turn, i, onto] = total.astype(bf16)
                for i in range(first, first + BATCH):
                    part_copy(turn, 2 if i % 2 == 0 else 1, i).start()

        either(kinds(SUM_DIRECT, turn), nothing, relays)

    def whole(ref, send_sem, recv_sem):
        return pltpu.make_async_remote_copy(
            src_ref=ref,
            dst_ref=ref,
            send_sem=send_sem,
            recv_sem=recv_sem,
            device_id={"orb": target(1)},
            device_id_type=pl.DeviceIdType.MESH,
        )

    def part_wait(turn, at):
        def wait(terms):
            arrived = parts_in.at[turn, at, pl.ds(0, terms)]
            whole(arrived, part_send.at[turn], part_recv.at[turn, at]).wait_recv()

        if square:
            either(kinds(SUM_DIRECT, turn), lambda: wait(3), lambda: wait(2))
        else:
            wait(ranks - 1)

    def sent(turn):
        sends = pl.ds(0, (ranks - 1) * own_pairs)
        whole(amps.at[turn, sends], amp_send.at[turn], amp_recv.at[turn, 0]).wait_send()
        sends = pl.ds(0, len(places) * orbs)
        whole(window.at[turn, sends], win_send.at[turn], win_recv.at[turn]).wait_send()

    def parts_sent(turn):
        whole(parts_in.at[turn], part_send.at[turn], part_recv.at[turn, 0]).wait_send()

    def amp_start(turn, i):
        for step in range(ranks - 1, 0, -1):
            amp_copy(turn, step, i).start()

    def amps_start(turn, batch, later=False):
        if square:
            if later and batch[0] >= BATCH:

                def far():
                    for i in batch:
                        amp_copy(turn, 3, i).start()

                either(direct_far, far, nothing)
            for turned in (0, 1):
                for i in batch:
                    amp_copy(turn, 1 if (i + turned) % 2 == 0 else 2, i).start()
        else:
            for i in batch:
                amp_start(turn, i)

    def win_start(turn, bare=False):
        win_copy(turn, c_place, bare).start()
        win_copy(turn, z_place, bare).start()

    def transposed(turn):
        for o in range(orbs):
            blocks_t[o] = window[turn, REACH * orbs + o].T

    def integral(turn, step, i):
        pair = target(step) * own_pairs + i
        left = blocks_t[occ_first[pair] % orbs]
        parts_out[turn, i, step] = dot(left, blocks[second_at[pair]]).astype(bf16)

    def integrals(turn):
        arrivals = window.at[turn, pl.ds(0, len(places) * orbs)]
        whole(arrivals, win_send.at[turn], win_recv.at[turn]).wait_recv()
        for at in range(SIDES * orbs):
            blocks[at] = window[turn, at]

        def one(i):
            for step in range(ranks - 1, -1, -1):
                integral(turn, step, i)
                if step > 0 and not square:
                    part_copy(turn, step, i).start()

        if square:
            for i in range(own_pairs):
                integral(turn, 3, i)
            for i in range(own_pairs):
                for step in (2, 1, 0):
                    integral(turn, step, i)
        else:
            pl.loop(0, own_pairs)(one)

    def far_sums(turn):
        def direct():
            for i in range(own_pairs):
                for step in (3, 1, 2):
                    part_copy(turn, step, i).start()

        def relays():
            for i in range(own_pairs):
                part_relay(turn, i).start()

        either(kinds(SUM_DIRECT, turn), direct, relays)

    def near_sums(turn):
        def relays():
            for i in range(own_pairs):
                part_copy(turn, 1 if i % 2 == 0 else 2, i).start()

        either(kinds(SUM_DIRECT, turn), nothing, relays)

    def through(turn, step):
        base = source(step) * own_pairs
        halves = []
        for i in range(own_pairs):
            amp = amps[turn, base + i]
            amps_now[base + i] = amp
            halves.append(dot(maps[base + i, 1], amp).astype(bf16))
        wholes = [dot(halves[i], first_t[base + i]) for i in range(own_pairs)]
        for i in range(own_pairs):
            local = occ_first[base + i] % orbs
            rows = pl.ds((step * own_pairs + i) * virtuals, virtuals)
            for o in range(orbs):
                masked = jnp.where(local == o, wholes[i], 0.0).astype(bf16)
                weights[rows, o * virtuals : (o + 1) * virtuals] = masked

    def applied(turn, some):
        lefts = [
            blocks[second_at[source(step) * own_pairs + i]]
            for step in some
            for i in range(own_pairs)
        ]
        rows = own_pairs * virtuals
        right = weights[pl.ds(some[0] * rows, len(some) * rows), :]
        return dot(jnp.concatenate(lefts, axis=1), right)

    def fit_near(turn):
        fitted[...] = applied(turn, near_steps)

    def dress(turn):
        if square:
            total = fitted[...] + applied(turn, far_steps)
        else:

            @pl.loop(1, ranks)
            def _(step):
                fitted[...] += applied(turn, (step,))

            total = fitted[...]
        values = [
            window[0, REACH * orbs + o].astype(jnp.float32)
            + dress_scale * total[:, o * virtuals : (o + 1) * virtuals]
            for o in range(orbs)
        ]

        @pl.when(turn + 1 < ITERS)
        def _():
            for o in range(orbs):
                window[turn + 1, REACH * orbs + o] = values[o].astype(bf16)

        @pl.when(turn + 1 == ITERS)
        def _():
            for o in range(orbs):
                out_dressed[o] = values[o]

    def couplings(turn):
        def one(i):
            halves = [
                dot(inter[i, k], amps_now[couple[i, k] % pairs]).astype(bf16)
                for k in range(partners)
            ]
            coupled[i] = dot(jnp.concatenate(halves, axis=1), inter_t[i])

        for i in range(own_pairs):
            one(i)

    def finish(turn):
        for first in range(0, own_pairs, BATCH):
            batch = range(first, min(first + BATCH, own_pairs))
            part_wait(turn, first // BATCH)
            totals = {}
            for i in batch:
                total = parts_out[turn, i, 0].astype(jnp.float32)
                for step in range(1, ranks if SUM_DIRECT != NONE or not square else 3):
                    total += parts_in[turn, i // BATCH, step - 1, i % BATCH].astype(jnp.float32)
                totals[i] = total.astype(bf16)
            rights = {i: dot(totals[i], maps[own + i, 1]).astype(bf16) for i in batch}
            values = {
                i: (dot(first_t[own + i], rights[i]) + coupled[i]) * scale[i] for i in batch
            }

            @pl.when(turn + 1 < ITERS)
            def _(batch=batch, values=values):
                for i in batch:
                    amps[turn + 1, own + i] = values[i].astype(bf16)
                amps_start(turn + 1, batch, True)

            @pl.when(turn + 1 == ITERS)
            def _(batch=batch, values=values):
                for i in batch:
                    out_amps[i] = values[i]

    win_start(0, True)
    orb_copy = pltpu.make_async_copy(orb_hbm, window.at[0, middle], orb_sem)
    orb_copy.start()
    small_copies[0].wait()
    for i in range(own_pairs):
        amps[0, own + i] = amplitudes[i].astype(bf16)
    amps_start(0, range(own_pairs))
    for copy in small_copies[1:]:
        copy.start()
    maps_copy = pltpu.make_async_copy(maps_hbm, maps, maps_sem)
    maps_copy.start()
    inter_copy = pltpu.make_async_copy(inter_hbm, inter, inter_sem)
    inter_copy.start()

    for copy in small_copies[1:]:
        copy.wait()

    @pl.loop(0, pairs)
    def _(pair):
        second = occ_second[pair]
        distance = (second // orbs - group + REACH + groups) % groups
        second_at[pair] = jnp.minimum(distance, SIDES - 1) * orbs + second % orbs

    if square and SUM_DIRECT != NONE:
        for turn in range(ITERS):

            def zero(turn=turn):
                for i in range(own_pairs):
                    parts_in[turn, i // BATCH, 2, i % BATCH] = jnp.zeros((size, size), bf16)

            either(kinds(SUM_DIRECT, turn), nothing, zero)

    orb_copy.wait()
    transposed(0)
    maps_copy.wait()

    @pl.loop(0, ranks)
    def _(block):
        for i in range(own_pairs):
            first_t[block * own_pairs + i] = maps[block * own_pairs + i, 0].T

    inter_copy.wait()

    @pl.loop(0, own_pairs)
    def _(i):
        rows = jnp.broadcast_to(pno_energy[pl.ds(i, 1), :], (size, size))
        denominator = rows + rows.T
        denominator -= occ_energy[occ_first[own + i]]
        denominator -= occ_energy[occ_second[own + i]]
        scale[i] = -1.0 / denominator
        for k in range(partners):
            inter_t[i, k * size : (k + 1) * size, :] = inter[i, k].T

    near_steps = (0, 1, 2) if square else (0,)
    far_steps = (3,) if square else tuple(range(1, ranks))

    def throughs(turn, some):
        first, last = some[0], some[-1] + 1
        if square and first > 0:
            amp_wait(turn, own_pairs + (0 if first == 1 else 1))

        @pl.loop(first, last)
        def _(step):
            if not square and first > 0:
                amp_wait(turn, step)
            through(turn, step)

    near_steps = (0, 1, 2) if square else (0,)
    far_steps = (3,) if square else tuple(range(1, ranks))
    throughs(0, (0,))
    relay_first = {"all": True, "inner": inner, "none": False}[FIRST_RELAY]
    if square:
        either(relay_first, lambda: relay_all(0), nothing)
        if EARLY_NEAR:
            either(inner, lambda: throughs(0, (1, 2)), nothing)

    def sums(turn, place):
        def some(far_place, near_place):
            if far_place == place:
                far_sums(turn)
            if near_place == place:
                near_sums(turn)

        either(inner, lambda: some(INNER_FAR, INNER_NEAR), lambda: some(0, 1))

    @pl.loop(0, ITERS)
    def _(turn):
        integrals(turn)

        if square:

            @pl.when(turn == 0)
            def _():
                far_sums(turn)
                if NEAR_AT == 0:
                    near_sums(turn)

            @pl.when(turn > 0)
            def _():
                sums(turn, 0)
                throughs(turn, (0,))
                relay_some(turn, range(BATCH))
                either(direct_far, nothing, lambda: relay_some(turn, beyond))
                sums(turn, 1)
                if FORWARD_EARLY:
                    either(inner, nothing, lambda: forward_all(turn))

                def late():
                    for i in beyond:
                        amp_copy(turn, 1 if i % 2 == 0 else 2, i).wait_recv()

                either(direct_far, late, nothing)

            if EARLY_NEAR:

                @pl.when(jnp.logical_or(turn > 0, jnp.logical_not(inner)))
                def _():
                    throughs(turn, (1, 2))

            else:
                throughs(turn, (1, 2))
        else:

            @pl.when(turn > 0)
            def _():
                throughs(turn, (0,))

        if square and not FORWARD_EARLY:

            @pl.when(jnp.logical_and(turn > 0, jnp.logical_not(inner)))
            def _():
                forward_all(turn)

        fit_near(turn)
        if square:

            @pl.when(turn > 0)
            def _():
                sums(turn, 2)

        throughs(turn, far_steps)
        dress(turn)

        @pl.when(turn + 1 < ITERS)
        def _():
            win_start(turn + 1)
            if square:
                if NEAR_AT == 1:
                    near_sums(turn)
                forward_all(turn)
                if NEAR_AT == 2:
                    near_sums(turn)
            transposed(turn + 1)

        if square:

            @pl.when(jnp.logical_and(turn > 0, inner))
            def _():
                forward_all(turn)

        couplings(turn)

        @pl.when(turn > 0)
        def _():
            sent(turn - 1)
            parts_sent(turn - 1)

        finish(turn)

    sent(ITERS - 1)
    parts_sent(ITERS - 1)


def store(amps, dressed, out_amps, out_dressed, sem):
    copies = [
        pltpu.make_async_copy(amps, out_amps, sem.at[0]),
        pltpu.make_async_copy(dressed, out_dressed, sem.at[1]),
    ]
    for copy in copies:
        copy.start()
    for copy in copies:
        copy.wait()


def on_device(
    ranks,
    groups,
    amplitudes,
    couple,
    occ_first,
    occ_second,
    couple_intersection,
    pno_maps,
    orbital_blocks,
    pno_energy,
    occ_energy,
):
    own_pairs, size, _ = amplitudes.shape
    group_pairs = occ_first.shape[0]
    orbs, rows, virtuals = orbital_blocks.shape
    partners = couple.shape[1]
    bf16 = jnp.bfloat16
    vmem = pl.BlockSpec(memory_space=pltpu.VMEM)
    hbm = pl.BlockSpec(memory_space=pltpu.HBM)
    dma = pltpu.SemaphoreType.DMA
    square = ranks == 4 and own_pairs % BATCH == 0
    results = pl.pallas_call(
        functools.partial(kernel, ranks, groups),
        out_shape=(
            pltpu.VMEM(amplitudes.shape, jnp.float32),
            pltpu.VMEM(orbital_blocks.shape, jnp.float32),
        ),
        in_specs=[hbm] * 9,
        out_specs=(vmem, vmem),
        scratch_shapes=[
            pltpu.SMEM(couple.shape, couple.dtype),
            pltpu.SMEM(occ_first.shape, occ_first.dtype),
            pltpu.SMEM(occ_second.shape, occ_second.dtype),
            pltpu.SMEM(occ_energy.shape, occ_energy.dtype),
            pltpu.SMEM(occ_second.shape, occ_second.dtype),
            pltpu.VMEM(amplitudes.shape, amplitudes.dtype),
            pltpu.VMEM(pno_energy.shape, pno_energy.dtype),
            pltpu.VMEM(couple_intersection.shape, bf16),
            pltpu.VMEM((own_pairs, partners * size, size), bf16),
            pltpu.VMEM(pno_maps.shape, bf16),
            pltpu.VMEM((group_pairs, size, virtuals), bf16),
            pltpu.VMEM((orbs, virtuals, rows), bf16),
            pltpu.VMEM((own_pairs, size, size), jnp.float32),
            pltpu.VMEM((own_pairs, size, size), jnp.float32),
            pltpu.VMEM((ITERS, group_pairs, size, size), bf16),
            pltpu.VMEM((group_pairs, size, size), bf16),
            pltpu.VMEM((ITERS, SIDES * orbs, rows, virtuals), bf16),
            pltpu.VMEM((SIDES * orbs, rows, virtuals), bf16),
            pltpu.VMEM((ITERS, own_pairs, ranks, virtuals, virtuals), bf16),
            pltpu.VMEM((ITERS, own_pairs // BATCH, ranks - 1, BATCH, virtuals, virtuals), bf16),
            pltpu.VMEM((ITERS, own_pairs, virtuals, virtuals), bf16),
            pltpu.VMEM((group_pairs * virtuals, orbs * virtuals), bf16),
            pltpu.VMEM((rows, orbs * virtuals), jnp.float32),
            dma((ITERS,)),
            dma((ITERS, own_pairs + 2 if square else ranks)),
            dma((ITERS,)),
            dma((ITERS,)),
            dma((ITERS,)),
            dma((ITERS, own_pairs // BATCH)),
            dma((ITERS, own_pairs // BATCH)),
            dma,
            dma,
            dma,
            dma((6,)),
        ],
        compiler_params=pltpu.CompilerParams(
            collective_id=0, has_side_effects=True, vmem_limit_bytes=67043328 - 4096 * 1024
        ),
    )(
        *(pltpu.with_memory_space_constraint(x, pltpu.HBM) for x in (
        couple,
        occ_first,
        occ_second,
        occ_energy,
        amplitudes,
        pno_energy,
        couple_intersection,
        pno_maps,
        orbital_blocks,
        ))
    )
    return pl.pallas_call(
        store,
        out_shape=tuple(pltpu.HBM(x.shape, x.dtype) for x in results),
        in_specs=[vmem] * 2,
        out_specs=(hbm, hbm),
        scratch_shapes=[dma((2,))],
        compiler_params=pltpu.CompilerParams(vmem_limit_bytes=4096 * 1024),
    )(*(pltpu.with_memory_space_constraint(x, pltpu.VMEM) for x in results))


def solution(mesh):
    return jax.shard_map(
        functools.partial(on_device, mesh.shape["orb"], mesh.shape["pair"]),
        mesh=mesh,
        in_specs=(
            P(("pair", "orb"), None, None),
            P(("pair", "orb"), None),
            P("pair"),
            P("pair"),
            P(("pair", "orb"), None, None, None),
            P("pair", None, None, None),
            P("pair", "orb", None),
            P(("pair", "orb"), None),
            P(),
        ),
        out_specs=(P(("pair", "orb"), None, None), P("pair", "orb", None)),
        check_vma=False,
    )
```
